128 devices in a mesh: member: 4 (over z), region: 32 (over y, x, core).
Axes of the slice: x: 4, y: 4, z: 4, core: 2. Of those that a mesh axis runs over, the one named last changes fastest.
Arguments:
- background: bfloat16 [64, 13, 192, 4096], P('member', None, 'region'), may hold values from -6 to 6
- obs_ens: bfloat16 [524288, 64], P(('member', 'region')), may hold values from -6 to 6
- obs_value: bfloat16 [524288], P(('member', 'region')), may hold values from -8 to 8
- obs_precision: bfloat16 [524288], P(('member', 'region')), may hold values from 0.0009994507 to 0.0099487305
- obs_row: int32 [524288], P(('member', 'region')), may hold values from 0 to 47
- obs_patch: int32 [524288, 1], P(('member', 'region')), may hold values from 0 to 127; in each aligned block of 4096 rows (0 to 4095, 4096 to 8191, ...) at most 64 rows name the same one
Outputs:
- analysis: bfloat16 [64, 13, 192, 4096], P(None, None, 'member', 'region')
The draws below stay inside these ranges and needn't reach their ends.
Inputs may be any that keep to these rules, and one draw needn't show every extreme that they name: `obs_patch`: among the observations of one device, at most 64 fall in one patch, and some patch receives exactly 64 of them.
All inputs are finite; a program needn't handle non-finite values.
Results may differ from the reference program's by a relative error of at most 0.0015.
The reference program's roundings to bfloat16 on the way count: a program that leaves them out, or rounds other values in their place, can miss the bound.
Values may be sent and summed in bfloat16 or wider, within the bound.
A program may use at most 128 MiB of HBM per device.

```python
import math
import jax
import jax.numpy as jnp
import numpy as np
from jax import lax

K = 64
C = 13
PLAT = 48
PLON = 128
BAND = 2
OBS_DEV = 4096
NS_ITERS = 4
CAP = 64
NPATCH = 128
NLAT = 192
NLON = 4096
NOBS = 524288
N_MEMBER = 4
N_REGION = 32


def place_ends(array, key, low, high):
    place = [jax.random.randint(jax.random.fold_in(key, axis), (), 0, length) for axis, length in enumerate(array.shape)]
    widest = array.shape.index(max(array.shape))
    next_to = place[:widest] + [(place[widest] + 1) % array.shape[widest]] + place[widest + 1:]
    return array.at[tuple(place)].set(low).at[tuple(next_to)].set(high)


def levels(rng, extent, split, smallest, high):
    def one(dim, parts):
        draws = jax.random.uniform(jax.random.fold_in(jax.random.fold_in(rng, 6), dim), (parts,), jnp.float32, smallest / len(split), high / len(split))
        return jnp.repeat(jnp.exp(draws), extent[dim] // parts).reshape((-1,) + (1,) * (len(extent) - dim - 1))

    gain = one(*split[0])
    for cut in split[1:]:
        gain = gain * one(*cut)
    return gain


def assign_block(own_key, own, number, rows, count, top, bound, lean):
    sequence = jax.random.permutation(own_key, count)
    packed, ordinary = shares(count, rows * top, bound, lean, True), shares(count, rows * top, bound, lean, False)
    places = jnp.arange(count)

    def named(tallies, turn):
        used = int((tallies > 0).sum())
        fixed = max(1, used // 4)
        moved = fixed + (places - fixed + turn * (used - fixed)) % max(1, count - fixed)
        return jnp.zeros((count,), jnp.int32).at[sequence[jnp.where(places < fixed, places, moved)]].set(jnp.asarray(tallies, jnp.int32))

    tallies = jnp.where(number % 4 == 0, named(packed, number // 4), named(ordinary, number - number // 4 - 1))
    mixed = jax.random.permutation(jax.random.fold_in(own, 3), count)
    source_of, sink = mixed[0:count // 2 * 2:2], mixed[1:count // 2 * 2:2]
    margin = jnp.minimum(tallies[source_of] - 1, bound - tallies[sink]) // 2
    margin = jnp.where((source_of == sequence[0]) | (sink == sequence[0]) | (tallies[sink] == 0), 0, jnp.maximum(margin, 0))
    moved = jax.random.randint(jax.random.fold_in(own, 4), (count // 2,), 0, 1 << 20) % (margin + 1)
    tallies = tallies.at[source_of].add(-moved).at[sink].add(moved)
    members = jnp.searchsorted(jnp.cumsum(tallies), jnp.arange(rows * top), side="right").astype(jnp.int32)
    table = members.reshape(top, rows).T
    table = table[jax.random.permutation(jax.random.fold_in(own, 1), rows)]
    turn = jax.random.randint(jax.random.fold_in(own, 2), (rows, 1), 0, top)
    return jnp.take_along_axis(table, (jnp.arange(top)[None, :] + turn) % top, axis=1)


def shares(number_of, total, bound, skew, full):
    weights = [(1 << 20) // math.isqrt(grade ** skew) + 1 for grade in range(1, number_of + 1)]
    largest = bound if full else min(bound, max(-(-total // number_of), total * weights[0] // sum(weights)))
    least = 1 if total - largest >= number_of - 1 else 0
    given, rest = [largest] + [least] * (number_of - 1), total - largest - least * (number_of - 1)
    while rest > 0:
        candidates = [i for i in range(1, number_of) if given[i] < largest] or [i for i in range(1, number_of) if given[i] < bound]
        pool, left = sum([weights[i] for i in candidates]), rest
        for i in candidates:
            more = min(bound - given[i], max(1, left * weights[i] // pool), rest)
            given[i] = given[i] + more
            rest = rest - more
    return np.array(given)


def centred(own_key, extent, deviation, most, split=(), kind=jnp.bfloat16):
    gain = levels(own_key, extent, split, -0.22, 0.18) if split else 1.0
    values = jax.random.normal(own_key, extent, jnp.float32) * deviation * gain
    return jnp.minimum(jnp.maximum(values, -most), most).astype(kind)


def setup_inputs(seed: int = 0) -> dict:
    key_list = jax.random.split(jax.random.key(seed), 7)
    background = centred(key_list[0], (K, C, NLAT, NLON), 1.0, 6.0, ((0, 4), (2, 32)))
    obs_ens = centred(key_list[1], (NOBS, K), 1.0, 6.0, ((0, 128),))
    obs_value = centred(key_list[2], (NOBS,), 2.0, 8.0, ((0, 128),))
    obs_precision = jnp.clip(jnp.exp(math.log(0.0099487305) - 2.2979944 * jax.random.uniform(key_list[3], (NOBS,), jnp.float32) ** levels(key_list[3], (NOBS,), ((0, 128),), -0.2, 0.2)), 0.0009994507, 0.0099487305).astype(jnp.bfloat16)
    obs_row = place_ends(jax.random.randint(key_list[4], (NOBS,), 0, PLAT), jax.random.fold_in(key_list[4], 1), 0, PLAT - 1).astype(jnp.int32)
    obs_patch_keys = jax.random.split(jax.random.fold_in(key_list[5], 1), NOBS // OBS_DEV)
    obs_patch_turns = jax.random.permutation(jax.random.fold_in(key_list[5], 3), NOBS // OBS_DEV)
    obs_patch = jax.vmap(lambda own, number: assign_block(jax.random.fold_in(key_list[5], 2), own, number, OBS_DEV, NPATCH, 1, CAP, 1))(obs_patch_keys, obs_patch_turns).reshape((NOBS, 1))
    return {"background": background, "obs_ens": obs_ens, "obs_value": obs_value, "obs_precision": obs_precision, "obs_row": obs_row, "obs_patch": obs_patch}


def batched(left, right):
    return jnp.einsum('bij,bjk->bik', left, right, precision=lax.Precision.HIGHEST)

def localize(row_float, obs_prec):
    centers = jnp.arange(PLAT // BAND, dtype=jnp.float32) * BAND + (BAND - 1) / 2.0
    distance = (row_float[None, :] - centers[:, None]) / (PLAT / 4.0)
    return obs_prec[None, :] * jnp.exp(-0.5 * distance * distance)

def band_transforms(ens_vals, obs_val, obs_prec, row_float):
    ens_float = ens_vals.astype(jnp.float32)
    ens_mean = lax.optimization_barrier(jnp.sum(ens_float, axis=1)) / K
    ens_pert = (ens_float - ens_mean[:, None]).astype(jnp.bfloat16)
    pert_float = ens_pert.astype(jnp.float32)
    innovation = obs_val - ens_mean
    weight = localize(row_float, obs_prec)

    def band_gram(band_weight):
        scaled = (band_weight[:, None] * pert_float).astype(jnp.bfloat16)
        return lax.dot_general(scaled, ens_pert, (((0,), (0,)), ((), ())), preferred_element_type=jnp.float32)
    gram_band = lax.map(band_gram, weight)
    projected = jnp.dot(weight * innovation[None, :], pert_float, precision=lax.Precision.HIGHEST)
    identity = jnp.eye(K, dtype=jnp.float32)
    system = (K - 1.0) * identity + gram_band
    norm_f = jnp.sqrt(lax.optimization_barrier(jnp.sum(system * system, axis=(1, 2))))
    root_iter = system / norm_f[:, None, None]
    inv_root = jnp.broadcast_to(identity, system.shape)
    for newton_step in range(NS_ITERS):
        middle = 1.5 * identity - 0.5 * batched(inv_root, root_iter)
        root_iter = batched(root_iter, middle)
        inv_root = batched(middle, inv_root)
    spread = jnp.sqrt((K - 1.0) / norm_f)[:, None, None] * inv_root
    inverse = batched(inv_root, inv_root) / norm_f[:, None, None]
    mean_shift = jnp.einsum('bjk,bk->bj', inverse, projected, precision=lax.Precision.HIGHEST)
    return (spread + mean_shift[:, :, None]).astype(jnp.bfloat16)

def update(patch_states, transform):
    state_mean = lax.optimization_barrier(jnp.sum(patch_states.astype(jnp.float32), axis=0)) / K
    state_pert = (patch_states.astype(jnp.float32) - state_mean[None]).astype(jnp.bfloat16)
    shaped = state_pert.reshape(K, C, PLAT // BAND, BAND, PLON).astype(jnp.float32)
    increment = jnp.einsum('jcbxl,bjk->kcbxl', shaped, transform.astype(jnp.float32))
    result = state_mean.reshape(1, C, PLAT // BAND, BAND, PLON) + increment
    return result.reshape(K, C, PLAT, PLON).astype(jnp.bfloat16)

def reference(background, obs_ens, obs_value, obs_precision, obs_row, obs_patch):
    target_patch = obs_patch[:, 0].astype(jnp.int32)
    ordering = jnp.argsort(target_patch, stable=True).astype(jnp.int32)
    counts = jax.ops.segment_sum(jnp.ones_like(target_patch), target_patch, NPATCH).astype(jnp.int32)
    starts = (jnp.cumsum(counts) - counts).astype(jnp.int32)
    room = NPATCH * CAP
    padded_order = jnp.concatenate([ordering, jnp.zeros((room,), jnp.int32)])

    def one_patch(patch_id):
        picked = lax.dynamic_slice_in_dim(padded_order, starts[patch_id], room)
        is_live = jnp.arange(room, dtype=jnp.int32) < counts[patch_id]
        ens_vals = jnp.where(is_live[:, None], obs_ens[picked], jnp.zeros((), jnp.bfloat16))
        obs_val = jnp.where(is_live, obs_value[picked].astype(jnp.float32), 0.0)
        obs_prec = jnp.where(is_live, obs_precision[picked].astype(jnp.float32), 0.0)
        row_float = obs_row[picked].astype(jnp.float32)
        transform = band_transforms(ens_vals, obs_val, obs_prec, row_float)
        lat_block = (patch_id // N_REGION).astype(jnp.int32)
        lon_block = (patch_id % N_REGION).astype(jnp.int32)
        zero = jnp.zeros((), jnp.int32)
        patch_states = lax.dynamic_slice(background, (zero, zero, lat_block * PLAT, lon_block * PLON), (K, C, PLAT, PLON))
        return update(patch_states, transform)
    patches = lax.map(one_patch, jnp.arange(NPATCH, dtype=jnp.int32))
    patches = patches.reshape(N_MEMBER, N_REGION, K, C, PLAT, PLON)
    return patches.transpose(2, 3, 0, 4, 1, 5).reshape(K, C, NLAT, NLON)
```

```python
import jax
import jax.numpy as jnp
from jax import lax
from jax.experimental import pallas as pl
from jax.experimental.pallas import tpu as pltpu
from jax.sharding import PartitionSpec as P

MESH = pl.DeviceIdType.MESH
F32 = jnp.float32
BF16 = jnp.bfloat16
HI = lax.Precision.HIGHEST

K = 64
C = 13
ROWS = 6
LON = 4096
OBS = 4096
CAP = 64
NB = 24
ND = 128
NS_ITERS = 4
EARLY = 3
PIECE = 40
CHUNK = 1024


def nt(a, b, **kw):
    return lax.dot_general(a, b, (((1,), (1,)), ((), ())), preferred_element_type=F32, **kw)


def kernel(bg, ens, ext, patch, out, in_all, stage, recv, flat, lhs, keys, obs_send, obs_recv, pert_t, weight, weighted,
           scaled, gram, proj, trans, wide, narrow, in_sem, send_sem, recv_sem, osend_sem, orecv_sem, oself_sem, out_sem):
    m = lax.axis_index("member")
    r = lax.axis_index("region")
    me = m * 32 + r
    y = r // 8
    xc = lax.rem(r, 8)
    x = xc // 2
    core = lax.rem(xc, 2)
    sign = 1 - 2 * core
    mine = m * 8 + xc

    @pl.loop(0, C)
    def _(ch):
        pltpu.make_async_copy(bg.at[:, ch], in_all.at[ch], in_sem.at[ch]).start()

    def relayout(ch):
        pltpu.make_async_copy(bg.at[:, ch], in_all.at[ch], in_sem.at[ch]).wait()

        @pl.loop(0, 16)
        def _(tt):
            for u in range(2):
                t = tt * 2 + u
                for mm in range(16):
                    piece = in_all[ch, mm, :, pl.ds(pl.multiple_of(t * 128, 128), 128)]
                    flat[u, pl.ds(mm * 8, ROWS), :] = piece.astype(F32)
            for u in range(2):
                t = tt * 2 + u
                for i in range(3):
                    pair = [flat[u, pl.ds(2 * i + h, 16, stride=8), :] for h in range(2)]
                    stage[ch, t, pl.ds(16 * i, 16), :] = jnp.concatenate(pair, axis=1).astype(BF16)

        @pl.when(m == y)
        def _():
            recv[ch, mine] = stage[ch, r]

    def send(ch):
        @pl.loop(0, 32)
        def _(k):
            q = lax.rem(k * 13 + ch * 7, 32)
            tx = lax.rem(x + sign * lax.rem(q // 2, 4) + 8, 4)
            ty = lax.rem(y + sign * (q // 8) + 8 + m, 4)
            tc = lax.rem(core + lax.rem(q, 2), 2)
            t = (ty * 4 + tx) * 2 + tc

            @pl.when(jnp.logical_or(t != r, m != y))
            def _():
                pltpu.make_async_remote_copy(
                    src_ref=stage.at[ch, t], dst_ref=recv.at[ch, mine],
                    send_sem=send_sem.at[ch], recv_sem=recv_sem.at[ch],
                    device_id=(y, t), device_id_type=MESH).start()

    def wait_blocks(ch, sem):
        @pl.when(m == y)
        def _():
            part = recv.at[ch, pl.ds(0, 31)]
            pltpu.make_async_copy(part, part, sem.at[ch]).wait()

        @pl.when(m != y)
        def _():
            pltpu.make_async_copy(recv.at[ch], recv.at[ch], sem.at[ch]).wait()

    relayout(0)

    @pl.loop(1, EARLY + 1)
    def _(ch):
        relayout(ch)
        send(ch - 1)

    lane = lax.broadcasted_iota(jnp.int32, (512, ND), 1)
    below = lax.broadcasted_iota(jnp.int32, (512, 512), 0) > lax.broadcasted_iota(jnp.int32, (512, 512), 1)
    lower = jnp.where(below, 1.0, 0.0).astype(BF16)

    def rank_block(b, before):
        at = pl.ds(pl.multiple_of(b * 512, 512), 512)
        col = patch[at, :]
        hit = jnp.where(col == lane, 1.0, 0.0)
        count = jnp.dot(lower, hit.astype(BF16), preferred_element_type=F32) + before
        rank = jnp.sum(count * hit, axis=1, keepdims=True).astype(jnp.int32)
        place = jnp.bitwise_and(col, 1) * CAP + rank
        tile = jnp.right_shift(col, 1).astype(F32)
        keys[at, :] = jnp.where(lane == place, tile, -1.0).astype(BF16)
        return before + jnp.sum(hit, axis=0, keepdims=True)

    lax.fori_loop(0, OBS // 512, rank_block, jnp.zeros((1, ND), F32))

    @pl.loop(0, OBS // 128)
    def _(i):
        at = pl.ds(pl.multiple_of(i * 128, 128), 128)
        lhs[0:K, at] = ens[at, :].astype(F32).T.astype(BF16)

    lhs[K:K + 16, :] = ext[...]

    half = lax.broadcasted_iota(jnp.int32, (32, 128), 1) < CAP
    half8 = lax.broadcasted_iota(jnp.int32, (8, 128), 1) < CAP

    def roll(v):
        return pltpu.roll(v, CAP, 1)

    @pl.loop(0, ND // 4)
    def _(g):
        total = jnp.zeros((K + 16, 256), F32)
        for kb in range(OBS // CHUNK):
            at = pl.ds(kb * CHUNK, CHUNK)
            key = keys[at, :]
            hot = [jnp.where(key == (2 * g + h).astype(F32).astype(BF16), 1.0, 0.0).astype(BF16) for h in range(2)]
            total += jnp.dot(lhs[:, at], jnp.concatenate(hot, axis=1), preferred_element_type=F32)
        for h in range(2):
            t = total[:, h * 128:(h + 1) * 128]
            low, high, more = t[0:32], t[32:64], t[64:72]
            first = jnp.concatenate([jnp.where(half, low, roll(high)), jnp.where(half8, more, 0.0)], axis=0)
            second = jnp.concatenate([jnp.where(half, roll(low), high), jnp.where(half8, roll(more), 0.0)], axis=0)
            obs_send[4 * g + 2 * h] = first.astype(BF16)
            obs_send[4 * g + 2 * h + 1] = second.astype(BF16)

    relayout(EARLY + 1)
    obs_recv[me] = obs_send[me]

    @pl.loop(1, ND)
    def _(d):
        to = lax.rem(me + lax.rem(d * 37, ND), ND)
        pltpu.make_async_remote_copy(
            src_ref=obs_send.at[to], dst_ref=obs_recv.at[me], send_sem=osend_sem, recv_sem=orecv_sem,
            device_id=(to // 32, lax.rem(to, 32)), device_id_type=MESH).start()

    send(EARLY)

    @pl.loop(EARLY + 2, C)
    def _(ch):
        relayout(ch)
        send(ch - 1)

    gram[...] = jnp.zeros_like(gram)
    proj[...] = jnp.zeros_like(proj)
    others = obs_recv.at[pl.ds(0, ND - 1)]
    pltpu.make_async_copy(others, others, orecv_sem).wait()
    send(C - 1)

    centre = lax.broadcasted_iota(jnp.int32, (NB, 128), 0).astype(F32) * 2.0 + 0.5

    @pl.loop(0, ND // 2)
    def _(p):
        at = pl.ds(pl.multiple_of(p * 128, 128), 128)
        a = obs_recv[2 * p].astype(F32)
        b = obs_recv[2 * p + 1].astype(F32)
        low = jnp.where(half, a[0:32], roll(b[0:32]))
        high = jnp.where(half, roll(a[0:32]), b[0:32])
        more = jnp.where(half8, a[32:40], roll(b[32:40]))
        values = jnp.concatenate([low, high], axis=0)
        mean = jnp.sum(values, axis=0, keepdims=True) / K
        pert_t[:, at] = (values - mean).astype(BF16)
        distance = (more[2:3] - centre) / 12.0
        w = more[1:2] * jnp.exp(-0.5 * distance * distance)
        weight[:, at] = w
        weighted[:, at] = w * (more[0:1] - mean)

    @pl.loop(0, ND * CAP // CHUNK)
    def _(kc):
        at = pl.ds(pl.multiple_of(kc * CHUNK, CHUNK), CHUNK)

        @pl.loop(0, NB)
        def _(j):
            w = weight[pl.ds(j, 1), at]
            scaled[pl.ds(pl.multiple_of(j * K, K), K), :] = (w * pert_t[:, at].astype(F32)).astype(BF16)

        gram[...] += nt(scaled[...], pert_t[:, at])
        proj[...] += nt(weighted[:, at], pert_t[:, at].astype(F32), precision=HI)

    eye = jnp.where(lax.broadcasted_iota(jnp.int32, (K, K), 0) == lax.broadcasted_iota(jnp.int32, (K, K), 1), 1.0, 0.0)

    def mm(a, b):
        return jnp.dot(a, b, precision=HI, preferred_element_type=F32)

    @pl.loop(0, NB // 4)
    def _(jj):
        group = range(4)
        sys_ = [gram[pl.ds(pl.multiple_of((jj * 4 + u) * K, K), K), :] + (K - 1.0) * eye for u in group]
        norm = [jnp.sqrt(jnp.sum(jnp.sum(s * s, axis=1, keepdims=True), axis=0, keepdims=True)) for s in sys_]
        root = [s / n for s, n in zip(sys_, norm)]
        middle = [1.5 * eye - 0.5 * a for a in root]
        root = [mm(a, b) for a, b in zip(root, middle)]
        inv = middle
        for step in range(1, NS_ITERS):
            middle = [1.5 * eye - 0.5 * mm(a, b) for a, b in zip(inv, root)]
            if step < NS_ITERS - 1:
                root = [mm(a, b) for a, b in zip(root, middle)]
            inv = [mm(a, b) for a, b in zip(middle, inv)]
        for u in group:
            inverse = mm(inv[u], inv[u]) / norm[u]
            shift = jnp.sum(inverse * proj[pl.ds(jj * 4 + u, 1), :], axis=1, keepdims=True)
            t = (jnp.sqrt((K - 1.0) / norm[u]) * inv[u] + shift)
            trans[jj * 4 + u] = t.T.astype(BF16)

    @pl.loop(0, C)
    def _(ch):
        wait_blocks(ch, recv_sem)
        slot = lax.rem(ch, 2)

        @pl.loop(0, 8)
        def _(s):
            for i in range(3):
                at = pl.ds(16 * i, 16)
                states = jnp.concatenate([recv[ch, z * 8 + s, at, :] for z in range(4)], axis=0).astype(F32)
                mean = jnp.sum(states, axis=0, keepdims=True) / K
                anomaly = (states - mean).astype(BF16)
                result = jnp.dot(trans[s * 3 + i], anomaly, preferred_element_type=F32) + mean
                wide[pl.ds(s * 6 + 2 * i, K, stride=48), :] = result[:, 0:128]
                wide[pl.ds(s * 6 + 2 * i + 1, K, stride=48), :] = result[:, 128:256]

        @pl.when(ch >= 2)
        def _():
            pltpu.make_async_copy(narrow.at[slot], out.at[:, ch], out_sem.at[slot]).wait()

        @pl.loop(0, K // 4)
        def _(k):
            for u in range(4):
                narrow[slot, k * 4 + u] = wide[pl.ds((k * 4 + u) * 48, 48), :].astype(BF16)

        pltpu.make_async_copy(narrow.at[slot], out.at[:, ch], out_sem.at[slot]).start()

    for slot in range(2):
        pltpu.make_async_copy(narrow.at[slot], out.at[:, 0], out_sem.at[slot]).wait()
    pltpu.make_async_copy(others, others, osend_sem).wait()

    @pl.loop(0, C)
    def _(ch):
        wait_blocks(ch, send_sem)


def local(background, obs_ens, obs_value, obs_precision, obs_row, obs_patch):
    zero = jnp.zeros_like(obs_value)
    ext = jnp.stack([obs_value, obs_precision, obs_row.astype(BF16)] + [zero] * 13, axis=0)
    vmem = pl.BlockSpec(memory_space=pltpu.VMEM)
    anyspace = pl.BlockSpec(memory_space=pl.ANY)
    return pl.pallas_call(
        kernel,
        out_shape=jax.ShapeDtypeStruct((K, C, 48, 128), BF16),
        in_specs=[anyspace, vmem, vmem, vmem],
        out_specs=anyspace,
        scratch_shapes=[
            pltpu.VMEM((C, 16, ROWS, LON), BF16),
            pltpu.VMEM((C, 32, 48, 256), BF16),
            pltpu.VMEM((C, 32, 48, 256), BF16),
            pltpu.VMEM((2, 128, 128), F32),
            pltpu.VMEM((K + 16, OBS), BF16),
            pltpu.VMEM((OBS, ND), BF16),
            pltpu.VMEM((ND, PIECE, 128), BF16),
            pltpu.VMEM((ND, PIECE, 128), BF16),
            pltpu.VMEM((K, ND * CAP), BF16),
            pltpu.VMEM((NB, ND * CAP), F32),
            pltpu.VMEM((NB, ND * CAP), F32),
            pltpu.VMEM((NB * K, CHUNK), BF16),
            pltpu.VMEM((NB * K, K), F32),
            pltpu.VMEM((NB, K), F32),
            pltpu.VMEM((NB, K, K), BF16),
            pltpu.VMEM((K * 48, 128), F32),
            pltpu.VMEM((2, K, 48, 128), BF16),
            pltpu.SemaphoreType.DMA((C,)),
            pltpu.SemaphoreType.DMA((C,)),
            pltpu.SemaphoreType.DMA((C,)),
            pltpu.SemaphoreType.DMA,
            pltpu.SemaphoreType.DMA,
            pltpu.SemaphoreType.DMA,
            pltpu.SemaphoreType.DMA((2,)),
        ],
        compiler_params=pltpu.CompilerParams(has_side_effects=True, vmem_limit_bytes=63 * 2**20),
        name="analysis",
    )(background, obs_ens, ext, obs_patch)


def solution(mesh):
    in_specs = (
        P("member", None, "region", None),
        P(("member", "region"), None),
        P(("member", "region")),
        P(("member", "region")),
        P(("member", "region")),
        P(("member", "region"), None),
    )
    out_specs = P(None, None, "member", "region")
    return jax.shard_map(local, mesh=mesh, in_specs=in_specs, out_specs=out_specs, check_vma=False)
```

```python
import jax
import jax.numpy as jnp
from jax import lax
from jax.experimental import pallas as pl
from jax.experimental.pallas import tpu as pltpu
from jax.sharding import PartitionSpec as P

MESH = pl.DeviceIdType.MESH
F32 = jnp.float32
BF16 = jnp.bfloat16
HI = lax.Precision.HIGHEST

K = 64
C = 13
ROWS = 6
LON = 4096
OBS = 4096
CAP = 64
NB = 24
ND = 128
NS_ITERS = 4
EARLY = 3
PIECE = 40
CHUNK = 1024


def nt(a, b, **kw):
    return lax.dot_general(a, b, (((1,), (1,)), ((), ())), preferred_element_type=F32, **kw)


def kernel(bg, ens, value, precision, row, patch, out, stage, recv, lines, lhs, keys, obs_send, obs_recv, pert_t, weight, weighted,
           scaled, gram, proj, trans, wide, narrow, in_sem, send_sem, recv_sem, osend_sem, orecv_sem, oself_sem, out_sem):
    m = lax.axis_index("member")
    r = lax.axis_index("region")
    me = m * 32 + r
    y = r // 8
    xc = lax.rem(r, 8)
    x = xc // 2
    core = lax.rem(xc, 2)
    sign = 1 - 2 * core
    mine = m * 8 + xc

    pltpu.make_async_copy(ens, lhs.at[pl.ds(0, K)], oself_sem).start()

    def block(ch, t):
        return bg.at[ch, :, :, pl.ds(pl.multiple_of(t * 128, 128), 128)]

    def fetch(ch):
        @pl.loop(0, 32)
        def _(t):
            pltpu.make_async_copy(block(ch, t), stage.at[ch, t], in_sem.at[ch]).start()

        @pl.when(m == y)
        def _():
            pltpu.make_async_copy(block(ch, r), recv.at[ch, mine], recv_sem.at[ch]).start()

    barrier = pltpu.get_barrier_semaphore()

    @pl.loop(1, ND)
    def _(d):
        to = lax.rem(me + d, ND)
        pl.semaphore_signal(barrier, inc=1, device_id=(to // 32, lax.rem(to, 32)), device_id_type=MESH)

    @pl.loop(0, C)
    def _(ch):
        fetch(ch)

    pl.semaphore_wait(barrier, ND - 1)

    def send(ch):
        pltpu.make_async_copy(recv.at[ch], stage.at[ch], in_sem.at[ch]).wait()

        @pl.loop(0, 32)
        def _(k):
            q = lax.rem(k * 13 + ch * 7, 32)
            tx = lax.rem(x + sign * lax.rem(q // 2, 4) + 8, 4)
            ty = lax.rem(y + sign * (q // 8) + 8 + m, 4)
            tc = lax.rem(core + lax.rem(q, 2), 2)
            t = (ty * 4 + tx) * 2 + tc

            @pl.when(jnp.logical_or(t != r, m != y))
            def _():
                pltpu.make_async_remote_copy(
                    src_ref=stage.at[ch, t], dst_ref=recv.at[ch, mine],
                    send_sem=send_sem.at[ch], recv_sem=recv_sem.at[ch],
                    device_id=(y, t), device_id_type=MESH).start()

    @pl.loop(0, EARLY)
    def _(ch):
        send(ch)

    above = lax.broadcasted_iota(jnp.int32, (512, 512), 0) < lax.broadcasted_iota(jnp.int32, (512, 512), 1)
    upper = jnp.where(above, 1.0, 0.0).astype(BF16)
    owner = lax.broadcasted_iota(jnp.int32, (ND, 128), 0)
    lane = lax.broadcasted_iota(jnp.int32, (128, 128), 1)

    def rank_block(b, before):
        rows = [patch[pl.ds(b * 4 + u, 1), :] for u in range(4)]
        hit = jnp.concatenate([jnp.where(owner == p, 1.0, 0.0) for p in rows], axis=1)
        count = jnp.dot(hit.astype(BF16), upper, preferred_element_type=F32) + before
        rank = jnp.sum(count * hit, axis=0, keepdims=True)
        for u in range(4):
            slot = rows[u].astype(F32) * CAP + rank[:, u * 128:(u + 1) * 128]
            column = jnp.broadcast_to(slot, (128, 128)).T.astype(jnp.int32)
            found = lane == jnp.bitwise_and(column, 127)
            key = jnp.where(found, jnp.right_shift(column, 7).astype(F32), -1.0)
            keys[pl.ds(pl.multiple_of((b * 4 + u) * 128, 128), 128), :] = key.astype(BF16)
        return before + jnp.sum(hit, axis=1, keepdims=True)

    lax.fori_loop(0, OBS // 512, rank_block, jnp.zeros((ND, 1), F32))

    lines[0] = value[...].astype(F32)
    lines[1] = precision[...].astype(F32)
    lines[2] = row[...].astype(F32)
    which = lax.broadcasted_iota(jnp.int32, (16, 128), 0)

    @pl.loop(0, OBS // 128)
    def _(i):
        at = pl.ds(pl.multiple_of(i * 128, 128), 128)
        one = pl.ds(i, 1)
        extra = jnp.where(which == 2, lines[2, one, :], 0.0)
        extra = jnp.where(which == 1, lines[1, one, :], extra)
        extra = jnp.where(which == 0, lines[0, one, :], extra)
        lhs[K:K + 16, at] = extra.astype(BF16)

    pltpu.make_async_copy(ens, lhs.at[pl.ds(0, K)], oself_sem).wait()

    half = lax.broadcasted_iota(jnp.int32, (32, 128), 1) < CAP
    half8 = lax.broadcasted_iota(jnp.int32, (8, 128), 1) < CAP

    def roll(v):
        return pltpu.roll(v, CAP, 1)

    @pl.loop(0, ND // 4)
    def _(g):
        total = jnp.zeros((K + 16, 256), F32)
        for kb in range(OBS // CHUNK):
            at = pl.ds(kb * CHUNK, CHUNK)
            key = keys[at, :]
            hot = [jnp.where(key == (2 * g + h).astype(F32).astype(BF16), 1.0, 0.0).astype(BF16) for h in range(2)]
            total += jnp.dot(lhs[:, at], jnp.concatenate(hot, axis=1), preferred_element_type=F32)
        for h in range(2):
            t = total[:, h * 128:(h + 1) * 128]
            low, high, more = t[0:32], t[32:64], t[64:72]
            first = jnp.concatenate([jnp.where(half, low, roll(high)), jnp.where(half8, more, 0.0)], axis=0)
            second = jnp.concatenate([jnp.where(half, roll(low), high), jnp.where(half8, roll(more), 0.0)], axis=0)
            obs_send[4 * g + 2 * h] = first.astype(BF16)
            obs_send[4 * g + 2 * h + 1] = second.astype(BF16)

    obs_recv[me] = obs_send[me]

    @pl.loop(1, ND)
    def _(d):
        to = lax.rem(me + lax.rem(d * 37, ND), ND)
        pltpu.make_async_remote_copy(
            src_ref=obs_send.at[to], dst_ref=obs_recv.at[me], send_sem=osend_sem, recv_sem=orecv_sem,
            device_id=(to // 32, lax.rem(to, 32)), device_id_type=MESH).start()

    gram[...] = jnp.zeros_like(gram)
    proj[...] = jnp.zeros_like(proj)
    others = obs_recv.at[pl.ds(0, ND - 1)]
    pltpu.make_async_copy(others, others, orecv_sem).wait()

    @pl.loop(EARLY, C)
    def _(ch):
        send(ch)

    centre = lax.broadcasted_iota(jnp.int32, (NB, 128), 0).astype(F32) * 2.0 + 0.5

    @pl.loop(0, ND // 2)
    def _(p):
        at = pl.ds(pl.multiple_of(p * 128, 128), 128)
        a = obs_recv[2 * p].astype(F32)
        b = obs_recv[2 * p + 1].astype(F32)
        low = jnp.where(half, a[0:32], roll(b[0:32]))
        high = jnp.where(half, roll(a[0:32]), b[0:32])
        more = jnp.where(half8, a[32:40], roll(b[32:40]))
        values = jnp.concatenate([low, high], axis=0)
        mean = jnp.sum(values, axis=0, keepdims=True) / K
        pert_t[:, at] = (values - mean).astype(BF16)
        distance = (more[2:3] - centre) / 12.0
        w = more[1:2] * jnp.exp(-0.5 * distance * distance)
        weight[:, at] = w
        weighted[:, at] = w * (more[0:1] - mean)

    @pl.loop(0, ND * CAP // CHUNK)
    def _(kc):
        at = pl.ds(pl.multiple_of(kc * CHUNK, CHUNK), CHUNK)

        @pl.loop(0, NB)
        def _(j):
            w = weight[pl.ds(j, 1), at]
            scaled[pl.ds(pl.multiple_of(j * K, K), K), :] = (w * pert_t[:, at].astype(F32)).astype(BF16)

        gram[...] += nt(scaled[...], pert_t[:, at])
        proj[...] += nt(weighted[:, at], pert_t[:, at].astype(F32), precision=HI)

    eye = jnp.where(lax.broadcasted_iota(jnp.int32, (K, K), 0) == lax.broadcasted_iota(jnp.int32, (K, K), 1), 1.0, 0.0)

    def mm(a, b):
        return jnp.dot(a, b, precision=HI, preferred_element_type=F32)

    @pl.loop(0, NB // 4)
    def _(jj):
        group = range(4)
        sys_ = [gram[pl.ds(pl.multiple_of((jj * 4 + u) * K, K), K), :] + (K - 1.0) * eye for u in group]
        norm = [jnp.sqrt(jnp.sum(jnp.sum(s * s, axis=1, keepdims=True), axis=0, keepdims=True)) for s in sys_]
        root = [s / n for s, n in zip(sys_, norm)]
        middle = [1.5 * eye - 0.5 * a for a in root]
        root = [mm(a, b) for a, b in zip(root, middle)]
        inv = middle
        for step in range(1, NS_ITERS):
            middle = [1.5 * eye - 0.5 * mm(a, b) for a, b in zip(inv, root)]
            if step < NS_ITERS - 1:
                root = [mm(a, b) for a, b in zip(root, middle)]
            inv = [mm(a, b) for a, b in zip(middle, inv)]
        for u in group:
            inverse = mm(inv[u], inv[u]) / norm[u]
            shift = jnp.sum(inverse * proj[pl.ds(jj * 4 + u, 1), :], axis=1, keepdims=True)
            t = (jnp.sqrt((K - 1.0) / norm[u]) * inv[u] + shift)
            trans[jj * 4 + u] = t.T.astype(BF16)

    @pl.loop(0, C)
    def _(ch):
        pltpu.make_async_copy(stage.at[ch], recv.at[ch], recv_sem.at[ch]).wait()
        slot = lax.rem(ch, 2)

        @pl.loop(0, 8)
        def _(s):
            for i in range(3):
                rows = [jnp.concatenate([recv[ch, z * 8 + s, 2 * i + h] for z in range(4)], axis=0) for h in range(2)]
                states = jnp.concatenate(rows, axis=1).astype(F32)
                mean = jnp.sum(states, axis=0, keepdims=True) / K
                anomaly = (states - mean).astype(BF16)
                result = jnp.dot(trans[s * 3 + i], anomaly, preferred_element_type=F32) + mean
                wide[pl.ds(s * 6 + 2 * i, K, stride=48), :] = result[:, 0:128]
                wide[pl.ds(s * 6 + 2 * i + 1, K, stride=48), :] = result[:, 128:256]

        @pl.when(ch >= 2)
        def _():
            pltpu.make_async_copy(narrow.at[slot], out.at[:, ch], out_sem.at[slot]).wait()

        @pl.loop(0, K // 4)
        def _(k):
            for u in range(4):
                narrow[slot, k * 4 + u] = wide[pl.ds((k * 4 + u) * 48, 48), :].astype(BF16)

        pltpu.make_async_copy(narrow.at[slot], out.at[:, ch], out_sem.at[slot]).start()

    for slot in range(2):
        pltpu.make_async_copy(narrow.at[slot], out.at[:, 0], out_sem.at[slot]).wait()
    pltpu.make_async_copy(others, others, osend_sem).wait()

    @pl.loop(0, C)
    def _(ch):
        @pl.when(m == y)
        def _():
            part = recv.at[ch, pl.ds(0, 31)]
            pltpu.make_async_copy(part, part, send_sem.at[ch]).wait()

        @pl.when(m != y)
        def _():
            pltpu.make_async_copy(recv.at[ch], recv.at[ch], send_sem.at[ch]).wait()


def local(background, obs_ens, obs_value, obs_precision, obs_row, obs_patch):
    lines = (OBS // 128, 128)
    operands = (
        background.transpose(1, 2, 0, 3), obs_ens.T, obs_value.reshape(lines), obs_precision.reshape(lines),
        obs_row.reshape(lines), obs_patch.reshape(lines),
    )
    vmem = pl.BlockSpec(memory_space=pltpu.VMEM)
    anyspace = pl.BlockSpec(memory_space=pl.ANY)
    return pl.pallas_call(
        kernel,
        out_shape=jax.ShapeDtypeStruct((K, C, 48, 128), BF16),
        in_specs=[anyspace, anyspace, vmem, vmem, vmem, vmem],
        out_specs=anyspace,
        scratch_shapes=[
            pltpu.VMEM((C, 32, ROWS, 16, 128), BF16),
            pltpu.VMEM((C, 32, ROWS, 16, 128), BF16),
            pltpu.VMEM((3, OBS // 128, 128), F32),
            pltpu.VMEM((K + 16, OBS), BF16),
            pltpu.VMEM((OBS, ND), BF16),
            pltpu.VMEM((ND, PIECE, 128), BF16),
            pltpu.VMEM((ND, PIECE, 128), BF16),
            pltpu.VMEM((K, ND * CAP), BF16),
            pltpu.VMEM((NB, ND * CAP), F32),
            pltpu.VMEM((NB, ND * CAP), F32),
            pltpu.VMEM((NB * K, CHUNK), BF16),
            pltpu.VMEM((NB * K, K), F32),
            pltpu.VMEM((NB, K), F32),
            pltpu.VMEM((NB, K, K), BF16),
            pltpu.VMEM((K * 48, 128), F32),
            pltpu.VMEM((2, K, 48, 128), BF16),
            pltpu.SemaphoreType.DMA((C,)),
            pltpu.SemaphoreType.DMA((C,)),
            pltpu.SemaphoreType.DMA((C,)),
            pltpu.SemaphoreType.DMA,
            pltpu.SemaphoreType.DMA,
            pltpu.SemaphoreType.DMA,
            pltpu.SemaphoreType.DMA((2,)),
        ],
        compiler_params=pltpu.CompilerParams(collective_id=0, has_side_effects=True, vmem_limit_bytes=63 * 2**20),
        name="analysis",
    )(*operands)


def solution(mesh):
    in_specs = (
        P("member", None, "region", None),
        P(("member", "region"), None),
        P(("member", "region")),
        P(("member", "region")),
        P(("member", "region")),
        P(("member", "region"), None),
    )
    out_specs = P(None, None, "member", "region")
    return jax.shard_map(local, mesh=mesh, in_specs=in_specs, out_specs=out_specs, check_vma=False)
```

```python
import jax
import jax.numpy as jnp
from jax import lax
from jax.experimental import pallas as pl
from jax.experimental.pallas import tpu as pltpu
from jax.sharding import PartitionSpec as P

MESH = pl.DeviceIdType.MESH
F32 = jnp.float32
BF16 = jnp.bfloat16
HI = lax.Precision.HIGHEST

K = 64
C = 13
ROWS = 6
LON = 4096
OBS = 4096
CAP = 64
NB = 24
ND = 128
NS_ITERS = 4
EARLY = 4
MID = 5
PIECE = 40
CHUNK = 1024


def nt(a, b, **kw):
    return lax.dot_general(a, b, (((1,), (1,)), ((), ())), preferred_element_type=F32, **kw)


def kernel(bg, ens, value, precision, row, patch, out, stage, recv, lines, lhs, keys, obs_send, obs_recv, pert_t, weight, weighted,
           scaled, gram, proj, trans, wide, in_sem, send_sem, recv_sem, osend_sem, orecv_sem, oself_sem):
    m = lax.axis_index("member")
    r = lax.axis_index("region")
    me = m * 32 + r
    y = r // 8
    xc = lax.rem(r, 8)
    x = xc // 2
    core = lax.rem(xc, 2)
    sign = 1 - 2 * core
    mine = m * 8 + xc

    pltpu.make_async_copy(ens, lhs.at[pl.ds(0, K)], oself_sem).start()

    def block(ch, t):
        return bg.at[ch, :, :, pl.ds(pl.multiple_of(t * 128, 128), 128)]

    def fetch(ch):
        @pl.loop(0, 32)
        def _(t):
            pltpu.make_async_copy(block(ch, t), stage.at[ch, t], in_sem.at[ch]).start()

        @pl.when(m == y)
        def _():
            pltpu.make_async_copy(block(ch, r), recv.at[ch, mine], recv_sem.at[ch]).start()

    barrier = pltpu.get_barrier_semaphore()

    @pl.loop(1, ND)
    def _(d):
        to = lax.rem(me + d, ND)
        pl.semaphore_signal(barrier, inc=1, device_id=(to // 32, lax.rem(to, 32)), device_id_type=MESH)

    @pl.loop(0, EARLY)
    def _(ch):
        fetch(ch)

    pl.semaphore_wait(barrier, ND - 1)

    def send(ch):
        pltpu.make_async_copy(recv.at[ch], stage.at[ch], in_sem.at[ch]).wait()

        @pl.loop(0, 32)
        def _(k):
            q = lax.rem(k * 13 + ch * 7, 32)
            tx = lax.rem(x + sign * lax.rem(q // 2, 4) + 8, 4)
            ty = lax.rem(y + sign * (q // 8) + 8 + m, 4)
            tc = lax.rem(core + lax.rem(q, 2), 2)
            t = (ty * 4 + tx) * 2 + tc

            @pl.when(jnp.logical_or(t != r, m != y))
            def _():
                pltpu.make_async_remote_copy(
                    src_ref=stage.at[ch, t], dst_ref=recv.at[ch, mine],
                    send_sem=send_sem.at[ch], recv_sem=recv_sem.at[ch],
                    device_id=(y, t), device_id_type=MESH).start()

    @pl.loop(0, EARLY)
    def _(ch):
        send(ch)

    @pl.loop(EARLY, C)
    def _(ch):
        fetch(ch)

    above = lax.broadcasted_iota(jnp.int32, (512, 512), 0) < lax.broadcasted_iota(jnp.int32, (512, 512), 1)
    upper = jnp.where(above, 1.0, 0.0).astype(BF16)
    owner = lax.broadcasted_iota(jnp.int32, (ND, 128), 0)
    lane = lax.broadcasted_iota(jnp.int32, (128, 128), 1)

    def rank_block(b, before):
        rows = [patch[pl.ds(b * 4 + u, 1), :] for u in range(4)]
        hit = jnp.concatenate([jnp.where(owner == p, 1.0, 0.0) for p in rows], axis=1)
        count = jnp.dot(hit.astype(BF16), upper, preferred_element_type=F32) + before
        rank = jnp.sum(count * hit, axis=0, keepdims=True)
        for u in range(4):
            slot = rows[u].astype(F32) * CAP + rank[:, u * 128:(u + 1) * 128]
            column = jnp.broadcast_to(slot, (128, 128)).T.astype(jnp.int32)
            found = lane == jnp.bitwise_and(column, 127)
            key = jnp.where(found, jnp.right_shift(column, 7).astype(F32), -1.0)
            keys[pl.ds(pl.multiple_of((b * 4 + u) * 128, 128), 128), :] = key.astype(BF16)
        return before + jnp.sum(hit, axis=1, keepdims=True)

    lax.fori_loop(0, OBS // 512, rank_block, jnp.zeros((ND, 1), F32))

    lines[0] = value[...].astype(F32)
    lines[1] = precision[...].astype(F32)
    lines[2] = row[...].astype(F32)
    which = lax.broadcasted_iota(jnp.int32, (16, 128), 0)

    @pl.loop(0, OBS // 128)
    def _(i):
        at = pl.ds(pl.multiple_of(i * 128, 128), 128)
        one = pl.ds(i, 1)
        extra = jnp.where(which == 2, lines[2, one, :], 0.0)
        extra = jnp.where(which == 1, lines[1, one, :], extra)
        extra = jnp.where(which == 0, lines[0, one, :], extra)
        lhs[K:K + 16, at] = extra.astype(BF16)

    pltpu.make_async_copy(ens, lhs.at[pl.ds(0, K)], oself_sem).wait()

    half = lax.broadcasted_iota(jnp.int32, (32, 128), 1) < CAP
    half8 = lax.broadcasted_iota(jnp.int32, (8, 128), 1) < CAP

    def roll(v):
        return pltpu.roll(v, CAP, 1)

    @pl.loop(0, ND // 4)
    def _(g):
        total = jnp.zeros((K + 16, 256), F32)
        for kb in range(OBS // CHUNK):
            at = pl.ds(kb * CHUNK, CHUNK)
            key = keys[at, :]
            hot = [jnp.where(key == (2 * g + h).astype(F32).astype(BF16), 1.0, 0.0).astype(BF16) for h in range(2)]
            total += jnp.dot(lhs[:, at], jnp.concatenate(hot, axis=1), preferred_element_type=F32)
        for h in range(2):
            t = total[:, h * 128:(h + 1) * 128]
            low, high, more = t[0:32], t[32:64], t[64:72]
            first = jnp.concatenate([jnp.where(half, low, roll(high)), jnp.where(half8, more, 0.0)], axis=0)
            second = jnp.concatenate([jnp.where(half, roll(low), high), jnp.where(half8, roll(more), 0.0)], axis=0)
            obs_send[4 * g + 2 * h] = first.astype(BF16)
            obs_send[4 * g + 2 * h + 1] = second.astype(BF16)

    obs_recv[me] = obs_send[me]

    @pl.loop(1, ND)
    def _(d):
        to = lax.rem(me + lax.rem(d * 37, ND), ND)
        pltpu.make_async_remote_copy(
            src_ref=obs_send.at[to], dst_ref=obs_recv.at[me], send_sem=osend_sem, recv_sem=orecv_sem,
            device_id=(to // 32, lax.rem(to, 32)), device_id_type=MESH).start()

    @pl.loop(EARLY, MID)
    def _(ch):
        send(ch)

    gram[...] = jnp.zeros_like(gram)
    proj[...] = jnp.zeros_like(proj)
    others = obs_recv.at[pl.ds(0, ND - 1)]
    pltpu.make_async_copy(others, others, orecv_sem).wait()

    @pl.loop(MID, C)
    def _(ch):
        send(ch)

    centre = lax.broadcasted_iota(jnp.int32, (NB, 128), 0).astype(F32) * 2.0 + 0.5

    @pl.loop(0, ND // 2)
    def _(p):
        at = pl.ds(pl.multiple_of(p * 128, 128), 128)
        a = obs_recv[2 * p].astype(F32)
        b = obs_recv[2 * p + 1].astype(F32)
        low = jnp.where(half, a[0:32], roll(b[0:32]))
        high = jnp.where(half, roll(a[0:32]), b[0:32])
        more = jnp.where(half8, a[32:40], roll(b[32:40]))
        values = jnp.concatenate([low, high], axis=0)
        mean = jnp.sum(values, axis=0, keepdims=True) / K
        pert_t[:, at] = (values - mean).astype(BF16)
        distance = (more[2:3] - centre) / 12.0
        w = more[1:2] * jnp.exp(-0.5 * distance * distance)
        weight[:, at] = w
        weighted[:, at] = w * (more[0:1] - mean)

    @pl.loop(0, ND * CAP // CHUNK)
    def _(kc):
        at = pl.ds(pl.multiple_of(kc * CHUNK, CHUNK), CHUNK)

        @pl.loop(0, NB)
        def _(j):
            w = weight[pl.ds(j, 1), at]
            scaled[pl.ds(pl.multiple_of(j * K, K), K), :] = (w * pert_t[:, at].astype(F32)).astype(BF16)

        gram[...] += nt(scaled[...], pert_t[:, at])
        proj[...] += nt(weighted[:, at], pert_t[:, at].astype(F32), precision=HI)

    eye = jnp.where(lax.broadcasted_iota(jnp.int32, (K, K), 0) == lax.broadcasted_iota(jnp.int32, (K, K), 1), 1.0, 0.0)

    def mm(a, b):
        return jnp.dot(a, b, precision=HI, preferred_element_type=F32)

    @pl.loop(0, NB // 4)
    def _(jj):
        group = range(4)
        sys_ = [gram[pl.ds(pl.multiple_of((jj * 4 + u) * K, K), K), :] + (K - 1.0) * eye for u in group]
        norm = [jnp.sqrt(jnp.sum(jnp.sum(s * s, axis=1, keepdims=True), axis=0, keepdims=True)) for s in sys_]
        root = [s / n for s, n in zip(sys_, norm)]
        middle = [1.5 * eye - 0.5 * a for a in root]
        root = [mm(a, b) for a, b in zip(root, middle)]
        inv = middle
        for step in range(1, NS_ITERS):
            middle = [1.5 * eye - 0.5 * mm(a, b) for a, b in zip(inv, root)]
            if step < NS_ITERS - 1:
                root = [mm(a, b) for a, b in zip(root, middle)]
            inv = [mm(a, b) for a, b in zip(middle, inv)]
        for u in group:
            inverse = mm(inv[u], inv[u]) / norm[u]
            shift = jnp.sum(inverse * proj[pl.ds(jj * 4 + u, 1), :], axis=1, keepdims=True)
            t = (jnp.sqrt((K - 1.0) / norm[u]) * inv[u] + shift)
            trans[jj * 4 + u] = t.T.astype(BF16)

    @pl.loop(0, C)
    def _(ch):
        pltpu.make_async_copy(stage.at[ch], recv.at[ch], recv_sem.at[ch]).wait()

        @pl.loop(0, 8)
        def _(s):
            for i in range(3):
                rows = [jnp.concatenate([recv[ch, z * 8 + s, 2 * i + h] for z in range(4)], axis=0) for h in range(2)]
                states = jnp.concatenate(rows, axis=1).astype(F32)
                mean = jnp.sum(states, axis=0, keepdims=True) / K
                anomaly = (states - mean).astype(BF16)
                result = jnp.dot(trans[s * 3 + i], anomaly, preferred_element_type=F32) + mean
                wide[pl.ds(s * 6 + 2 * i, K, stride=48), :] = result[:, 0:128]
                wide[pl.ds(s * 6 + 2 * i + 1, K, stride=48), :] = result[:, 128:256]

        @pl.loop(0, K // 4)
        def _(k):
            for u in range(4):
                out[k * 4 + u, ch] = wide[pl.ds((k * 4 + u) * 48, 48), :].astype(BF16)

    pltpu.make_async_copy(others, others, osend_sem).wait()

    @pl.loop(0, C)
    def _(ch):
        @pl.when(m == y)
        def _():
            part = recv.at[ch, pl.ds(0, 31)]
            pltpu.make_async_copy(part, part, send_sem.at[ch]).wait()

        @pl.when(m != y)
        def _():
            pltpu.make_async_copy(recv.at[ch], recv.at[ch], send_sem.at[ch]).wait()


def put(source, target, sem):
    @pl.loop(0, K // 4)
    def _(k):
        part = pl.ds(k * 4, 4)
        pltpu.make_async_copy(source.at[part], target.at[part], sem).start()

    pltpu.make_async_copy(source, target, sem).wait()


def local(background, obs_ens, obs_value, obs_precision, obs_row, obs_patch):
    lines = (OBS // 128, 128)
    operands = (
        background.transpose(1, 2, 0, 3), obs_ens.T, obs_value.reshape(lines), obs_precision.reshape(lines),
        obs_row.reshape(lines), obs_patch.reshape(lines),
    )
    vmem = pl.BlockSpec(memory_space=pltpu.VMEM)
    anyspace = pl.BlockSpec(memory_space=pl.ANY)
    result = pl.pallas_call(
        kernel,
        out_shape=jax.ShapeDtypeStruct((K, C, 48, 128), BF16),
        in_specs=[anyspace, anyspace, vmem, vmem, vmem, vmem],
        out_specs=vmem,
        scratch_shapes=[
            pltpu.VMEM((C, 32, ROWS, 16, 128), BF16),
            pltpu.VMEM((C, 32, ROWS, 16, 128), BF16),
            pltpu.VMEM((3, OBS // 128, 128), F32),
            pltpu.VMEM((K + 16, OBS), BF16),
            pltpu.VMEM((OBS, ND), BF16),
            pltpu.VMEM((ND, PIECE, 128), BF16),
            pltpu.VMEM((ND, PIECE, 128), BF16),
            pltpu.VMEM((K, ND * CAP), BF16),
            pltpu.VMEM((NB, ND * CAP), F32),
            pltpu.VMEM((NB, ND * CAP), F32),
            pltpu.VMEM((NB * K, CHUNK), BF16),
            pltpu.VMEM((NB * K, K), F32),
            pltpu.VMEM((NB, K), F32),
            pltpu.VMEM((NB, K, K), BF16),
            pltpu.VMEM((K * 48, 128), F32),
            pltpu.SemaphoreType.DMA((C,)),
            pltpu.SemaphoreType.DMA((C,)),
            pltpu.SemaphoreType.DMA((C,)),
            pltpu.SemaphoreType.DMA,
            pltpu.SemaphoreType.DMA,
            pltpu.SemaphoreType.DMA,
        ],
        compiler_params=pltpu.CompilerParams(collective_id=0, has_side_effects=True, vmem_limit_bytes=42 * 2**20),
        name="analysis",
    )(*operands)
    return pl.pallas_call(
        put,
        out_shape=jax.ShapeDtypeStruct((K, C, 48, 128), BF16),
        in_specs=[vmem],
        out_specs=anyspace,
        scratch_shapes=[pltpu.SemaphoreType.DMA],
        compiler_params=pltpu.CompilerParams(vmem_limit_bytes=2**20),
        name="put",
    )(result)


def solution(mesh):
    in_specs = (
        P("member", None, "region", None),
        P(("member", "region"), None),
        P(("member", "region")),
        P(("member", "region")),
        P(("member", "region")),
        P(("member", "region"), None),
    )
    out_specs = P(None, None, "member", "region")
    return jax.shard_map(local, mesh=mesh, in_specs=in_specs, out_specs=out_specs, check_vma=False)
```

```python
import jax
import jax.numpy as jnp
from jax import lax
from jax.experimental import pallas as pl
from jax.experimental.pallas import tpu as pltpu
from jax.sharding import PartitionSpec as P

MESH = pl.DeviceIdType.MESH
F32 = jnp.float32
BF16 = jnp.bfloat16
HI = lax.Precision.HIGHEST

K = 64
C = 13
ROWS = 6
LON = 4096
OBS = 4096
CAP = 64
NB = 24
ND = 128
NS_ITERS = 4
EARLY = 4
MID = 5
PIECE = 40
SENT = 34
CHUNK = 1024


def nt(a, b, **kw):
    return lax.dot_general(a, b, (((1,), (1,)), ((), ())), preferred_element_type=F32, **kw)


def kernel(bg, ens, value_in, precision_in, row_in, patch_in, out, stage, recv, value, precision, row, patch, lines, lhs, keys, obs_send, obs_recv, pert_t, weight, weighted,
           scaled, gram, proj, trans, wide, in_sem, send_sem, recv_sem, osend_sem, orecv_sem, oself_sem, small_sem):
    m = lax.axis_index("member")
    r = lax.axis_index("region")
    me = m * 32 + r
    y = r // 8
    xc = lax.rem(r, 8)
    x = xc // 2
    core = lax.rem(xc, 2)
    sign = 1 - 2 * core
    mine = m * 8 + xc

    small = ((value_in, value), (precision_in, precision), (row_in, row), (patch_in, patch))

    def block(ch, t):
        return bg.at[ch, :, :, pl.ds(pl.multiple_of(t * 128, 128), 128)]

    def fetch(ch):
        @pl.loop(0, 32)
        def _(t):
            pltpu.make_async_copy(block(ch, t), stage.at[ch, t], in_sem.at[ch]).start()

        @pl.when(m == y)
        def _():
            pltpu.make_async_copy(block(ch, r), recv.at[ch, mine], recv_sem.at[ch]).start()

    barrier = pltpu.get_barrier_semaphore()

    @pl.loop(2, 6)
    def _(dz):
        tz = jnp.bitwise_and(m + dz, 3)
        for dy in (2, 3, 1, 0):
            ty = jnp.bitwise_and(y + dy, 3) * 8
            for dx in (2, 3, 1, 0):
                tx = ty + jnp.bitwise_and(x + dx, 3) * 2
                for dc in (1, 0):
                    def greet():
                        pl.semaphore_signal(
                            barrier, inc=1, device_id=(tz, tx + jnp.bitwise_xor(core, dc)), device_id_type=MESH)
                    if dy == dx == dc == 0:
                        pl.when(dz != 4)(greet)
                    else:
                        greet()

    @pl.loop(0, EARLY)
    def _(ch):
        fetch(ch)

    pltpu.make_async_copy(ens, lhs.at[pl.ds(0, K)], oself_sem).start()
    for n, (source, target) in enumerate(small):
        pltpu.make_async_copy(source, target, small_sem.at[n]).start()

    pl.semaphore_wait(barrier, ND - 1)

    def send(ch):
        pltpu.make_async_copy(recv.at[ch], stage.at[ch], in_sem.at[ch]).wait()

        @pl.loop(0, 32)
        def _(k):
            q = lax.rem(k * 5 + ch * 3, 32)
            tx = lax.rem(x + sign * lax.rem(q // 2, 4) + 8, 4)
            ty = lax.rem(y + sign * (q // 8) + 8 + m, 4)
            tc = lax.rem(core + lax.rem(q, 2), 2)
            t = (ty * 4 + tx) * 2 + tc

            @pl.when(jnp.logical_or(t != r, m != y))
            def _():
                pltpu.make_async_remote_copy(
                    src_ref=stage.at[ch, t], dst_ref=recv.at[ch, mine],
                    send_sem=send_sem.at[ch], recv_sem=recv_sem.at[ch],
                    device_id=(y, t), device_id_type=MESH).start()

    @pl.loop(0, EARLY)
    def _(ch):
        send(ch)

    @pl.loop(EARLY, C)
    def _(ch):
        fetch(ch)

    for n, (source, target) in enumerate(small):
        pltpu.make_async_copy(source, target, small_sem.at[n]).wait()

    above = lax.broadcasted_iota(jnp.int32, (512, 512), 0) < lax.broadcasted_iota(jnp.int32, (512, 512), 1)
    upper = jnp.where(above, 1.0, 0.0).astype(BF16)
    owner = lax.broadcasted_iota(jnp.int32, (ND, 128), 0)
    lane = lax.broadcasted_iota(jnp.int32, (128, 128), 1)

    def rank_block(b, before):
        rows = [patch[pl.ds(b * 4 + u, 1), :] for u in range(4)]
        hit = jnp.concatenate([jnp.where(owner == p, 1.0, 0.0) for p in rows], axis=1)
        count = jnp.dot(hit.astype(BF16), upper, preferred_element_type=F32) + before
        rank = jnp.sum(count * hit, axis=0, keepdims=True)
        for u in range(4):
            slot = rows[u].astype(F32) * CAP + rank[:, u * 128:(u + 1) * 128]
            column = jnp.broadcast_to(slot, (128, 128)).T.astype(jnp.int32)
            found = lane == jnp.bitwise_and(column, 127)
            key = jnp.where(found, jnp.right_shift(column, 7).astype(F32), -1.0)
            keys[pl.ds(pl.multiple_of((b * 4 + u) * 128, 128), 128), :] = key.astype(BF16)
        return before + jnp.sum(hit, axis=1, keepdims=True)

    lax.fori_loop(0, OBS // 512, rank_block, jnp.zeros((ND, 1), F32))

    lines[0] = value[...].astype(F32)
    lines[1] = precision[...].astype(F32)
    lines[2] = row[...].astype(F32)
    which = lax.broadcasted_iota(jnp.int32, (16, 128), 0)

    @pl.loop(0, OBS // 128)
    def _(i):
        at = pl.ds(pl.multiple_of(i * 128, 128), 128)
        one = pl.ds(i, 1)
        extra = jnp.where(which == 2, lines[2, one, :], 0.0)
        extra = jnp.where(which == 1, lines[1, one, :], extra)
        extra = jnp.where(which == 0, lines[0, one, :], extra)
        lhs[K:K + 16, at] = extra.astype(BF16)

    pltpu.make_async_copy(ens, lhs.at[pl.ds(0, K)], oself_sem).wait()

    half = lax.broadcasted_iota(jnp.int32, (32, 128), 1) < CAP
    half8 = lax.broadcasted_iota(jnp.int32, (8, 128), 1) < CAP

    line8 = lax.broadcasted_iota(jnp.int32, (8, 128), 0)

    def roll(v):
        return pltpu.roll(v, CAP, 1)

    @pl.loop(0, ND // 4)
    def _(g):
        total = jnp.zeros((K + 16, 256), F32)
        for kb in range(OBS // CHUNK):
            at = pl.ds(kb * CHUNK, CHUNK)
            key = keys[at, :]
            hot = [jnp.where(key == (2 * g + h).astype(F32).astype(BF16), 1.0, 0.0).astype(BF16) for h in range(2)]
            total += jnp.dot(lhs[:, at], jnp.concatenate(hot, axis=1), preferred_element_type=F32)
        for h in range(2):
            t = total[:, h * 128:(h + 1) * 128]
            low, high, more = t[0:32], t[32:64], t[64:72]
            swapped = roll(more)
            line = jnp.where(half8[0:1], more[0:1], swapped[1:2])
            tail = jnp.where(line8 == 0, line, jnp.where(half8, more[2:3], 0.0))
            first = jnp.concatenate([jnp.where(half, low, roll(high)), tail], axis=0)
            line = jnp.where(half8[0:1], swapped[0:1], more[1:2])
            tail = jnp.where(line8 == 0, line, jnp.where(half8, swapped[2:3], 0.0))
            second = jnp.concatenate([jnp.where(half, roll(low), high), tail], axis=0)
            obs_send[4 * g + 2 * h] = first.astype(BF16)
            obs_send[4 * g + 2 * h + 1] = second.astype(BF16)

    obs_recv[me] = obs_send[me]

    @pl.loop(1, ND)
    def _(d):
        to = lax.rem(me + lax.rem(d * 37, ND), ND)
        pltpu.make_async_remote_copy(
            src_ref=obs_send.at[to, pl.ds(0, SENT)], dst_ref=obs_recv.at[me, pl.ds(0, SENT)], send_sem=osend_sem, recv_sem=orecv_sem,
            device_id=(to // 32, lax.rem(to, 32)), device_id_type=MESH).start()

    @pl.loop(EARLY, MID)
    def _(ch):
        send(ch)

    gram[...] = jnp.zeros_like(gram)
    proj[...] = jnp.zeros_like(proj)
    others = obs_recv.at[pl.ds(0, ND - 1), pl.ds(0, SENT)]
    pltpu.make_async_copy(others, others, orecv_sem).wait()

    @pl.loop(MID, C)
    def _(ch):
        send(ch)

    centre = lax.broadcasted_iota(jnp.int32, (NB, 128), 0).astype(F32) * 2.0 + 0.5

    @pl.loop(0, ND // 2)
    def _(p):
        at = pl.ds(pl.multiple_of(p * 128, 128), 128)
        a = obs_recv[2 * p].astype(F32)
        b = obs_recv[2 * p + 1].astype(F32)
        low = jnp.where(half, a[0:32], roll(b[0:32]))
        high = jnp.where(half, roll(a[0:32]), b[0:32])
        here = half8[0:1]
        ea, eb = a[32:40], b[32:40]
        ra, rb = roll(ea), roll(eb)
        obs_val = jnp.where(here, ea[0:1], rb[0:1])
        obs_prec = jnp.where(here, ra[0:1], eb[0:1])
        obs_row = jnp.where(here, ea[1:2], rb[1:2])
        values = jnp.concatenate([low, high], axis=0)
        mean = jnp.sum(values, axis=0, keepdims=True) / K
        pert_t[:, at] = (values - mean).astype(BF16)
        distance = (obs_row - centre) / 12.0
        w = obs_prec * jnp.exp(-0.5 * distance * distance)
        weight[:, at] = w
        weighted[:, at] = w * (obs_val - mean)

    @pl.loop(0, ND * CAP // CHUNK)
    def _(kc):
        at = pl.ds(pl.multiple_of(kc * CHUNK, CHUNK), CHUNK)

        @pl.loop(0, NB)
        def _(j):
            w = weight[pl.ds(j, 1), at]
            scaled[pl.ds(pl.multiple_of(j * K, K), K), :] = (w * pert_t[:, at].astype(F32)).astype(BF16)

        gram[...] += nt(scaled[...], pert_t[:, at])
        proj[...] += nt(weighted[:, at], pert_t[:, at].astype(F32), precision=HI)

    eye = jnp.where(lax.broadcasted_iota(jnp.int32, (K, K), 0) == lax.broadcasted_iota(jnp.int32, (K, K), 1), 1.0, 0.0)

    def mm(a, b):
        return jnp.dot(a, b, precision=HI, preferred_element_type=F32)

    @pl.loop(0, NB // 4)
    def _(jj):
        group = range(4)
        sys_ = [gram[pl.ds(pl.multiple_of((jj * 4 + u) * K, K), K), :] + (K - 1.0) * eye for u in group]
        norm = [jnp.sqrt(jnp.sum(jnp.sum(s * s, axis=1, keepdims=True), axis=0, keepdims=True)) for s in sys_]
        root = [s / n for s, n in zip(sys_, norm)]
        middle = [1.5 * eye - 0.5 * a for a in root]
        root = [mm(a, b) for a, b in zip(root, middle)]
        inv = middle
        for step in range(1, NS_ITERS):
            middle = [1.5 * eye - 0.5 * mm(a, b) for a, b in zip(inv, root)]
            if step < NS_ITERS - 1:
                root = [mm(a, b) for a, b in zip(root, middle)]
            inv = [mm(a, b) for a, b in zip(middle, inv)]
        for u in group:
            inverse = mm(inv[u], inv[u]) / norm[u]
            shift = jnp.sum(inverse * proj[pl.ds(jj * 4 + u, 1), :], axis=1, keepdims=True)
            t = (jnp.sqrt((K - 1.0) / norm[u]) * inv[u] + shift)
            trans[jj * 4 + u] = t.T.astype(BF16)

    @pl.loop(0, C)
    def _(ch):
        pltpu.make_async_copy(stage.at[ch], recv.at[ch], recv_sem.at[ch]).wait()

        @pl.loop(0, 8)
        def _(s):
            for i in range(3):
                rows = [jnp.concatenate([recv[ch, z * 8 + s, 2 * i + h] for z in range(4)], axis=0) for h in range(2)]
                states = jnp.concatenate(rows, axis=1).astype(F32)
                mean = jnp.sum(states, axis=0, keepdims=True) / K
                anomaly = (states - mean).astype(BF16)
                result = jnp.dot(trans[s * 3 + i], anomaly, preferred_element_type=F32) + mean
                wide[pl.ds(s * 6 + 2 * i, K, stride=48), :] = result[:, 0:128]
                wide[pl.ds(s * 6 + 2 * i + 1, K, stride=48), :] = result[:, 128:256]

        @pl.loop(0, K // 4)
        def _(k):
            for u in range(4):
                out[k * 4 + u, ch] = wide[pl.ds((k * 4 + u) * 48, 48), :].astype(BF16)

    pltpu.make_async_copy(others, others, osend_sem).wait()

    @pl.loop(0, C)
    def _(ch):
        @pl.when(m == y)
        def _():
            part = recv.at[ch, pl.ds(0, 31)]
            pltpu.make_async_copy(part, part, send_sem.at[ch]).wait()

        @pl.when(m != y)
        def _():
            pltpu.make_async_copy(recv.at[ch], recv.at[ch], send_sem.at[ch]).wait()


def put(source, target, sem):
    @pl.loop(0, K // 4)
    def _(k):
        part = pl.ds(k * 4, 4)
        pltpu.make_async_copy(source.at[part], target.at[part], sem).start()

    pltpu.make_async_copy(source, target, sem).wait()


def local(background, obs_ens, obs_value, obs_precision, obs_row, obs_patch):
    lines = (OBS // 128, 128)
    operands = (
        background.transpose(1, 2, 0, 3), obs_ens.T, obs_value.reshape(lines), obs_precision.reshape(lines),
        obs_row.reshape(lines), obs_patch.reshape(lines),
    )
    vmem = pl.BlockSpec(memory_space=pltpu.VMEM)
    hbm = pl.BlockSpec(memory_space=pltpu.HBM)
    anyspace = pl.BlockSpec(memory_space=pl.ANY)
    result = pl.pallas_call(
        kernel,
        out_shape=jax.ShapeDtypeStruct((K, C, 48, 128), BF16),
        in_specs=[hbm] * 6,
        out_specs=vmem,
        scratch_shapes=[
            pltpu.VMEM((C, 32, ROWS, 16, 128), BF16),
            pltpu.VMEM((C, 32, ROWS, 16, 128), BF16),
            pltpu.VMEM(lines, BF16),
            pltpu.VMEM(lines, BF16),
            pltpu.VMEM(lines, jnp.int32),
            pltpu.VMEM(lines, jnp.int32),
            pltpu.VMEM((3, OBS // 128, 128), F32),
            pltpu.VMEM((K + 16, OBS), BF16),
            pltpu.VMEM((OBS, ND), BF16),
            pltpu.VMEM((ND, PIECE, 128), BF16),
            pltpu.VMEM((ND, PIECE, 128), BF16),
            pltpu.VMEM((K, ND * CAP), BF16),
            pltpu.VMEM((NB, ND * CAP), F32),
            pltpu.VMEM((NB, ND * CAP), F32),
            pltpu.VMEM((NB * K, CHUNK), BF16),
            pltpu.VMEM((NB * K, K), F32),
            pltpu.VMEM((NB, K), F32),
            pltpu.VMEM((NB, K, K), BF16),
            pltpu.VMEM((K * 48, 128), F32),
            pltpu.SemaphoreType.DMA((C,)),
            pltpu.SemaphoreType.DMA((C,)),
            pltpu.SemaphoreType.DMA((C,)),
            pltpu.SemaphoreType.DMA,
            pltpu.SemaphoreType.DMA,
            pltpu.SemaphoreType.DMA,
            pltpu.SemaphoreType.DMA((4,)),
        ],
        compiler_params=pltpu.CompilerParams(collective_id=0, has_side_effects=True, vmem_limit_bytes=42 * 2**20),
        name="analysis",
    )(*[pltpu.with_memory_space_constraint(o, pltpu.HBM) for o in operands])
    return pl.pallas_call(
        put,
        out_shape=jax.ShapeDtypeStruct((K, C, 48, 128), BF16),
        in_specs=[vmem],
        out_specs=anyspace,
        scratch_shapes=[pltpu.SemaphoreType.DMA],
        compiler_params=pltpu.CompilerParams(vmem_limit_bytes=2**20),
        name="put",
    )(result)


def solution(mesh):
    in_specs = (
        P("member", None, "region", None),
        P(("member", "region"), None),
        P(("member", "region")),
        P(("member", "region")),
        P(("member", "region")),
        P(("member", "region"), None),
    )
    out_specs = P(None, None, "member", "region")
    return jax.shard_map(local, mesh=mesh, in_specs=in_specs, out_specs=out_specs, check_vma=False)
```

```python
import jax
import jax.numpy as jnp
from jax import lax
from jax.experimental import pallas as pl
from jax.experimental.pallas import tpu as pltpu
from jax.sharding import PartitionSpec as P

MESH = pl.DeviceIdType.MESH
F32 = jnp.float32
BF16 = jnp.bfloat16
HI = lax.Precision.HIGHEST

K = 64
C = 13
ROWS = 6
LON = 4096
OBS = 4096
CAP = 64
NB = 24
ND = 128
NS_ITERS = 4
EARLY = 4
MID = 5
PIECE = 40
SENT = 34
CHUNK = 1024


def nt(a, b, **kw):
    return lax.dot_general(a, b, (((1,), (1,)), ((), ())), preferred_element_type=F32, **kw)


def kernel(bg, ens, value_in, precision_in, row_in, patch_in, out, stage, recv, value, precision, row, patch, lines, lhs, keys, obs_send, obs_recv, pert_t, weight, weighted,
           scaled, gram, proj, trans, wide, in_sem, send_sem, recv_sem, osend_sem, orecv_sem, oself_sem, small_sem):
    m = lax.axis_index("member")
    r = lax.axis_index("region")
    me = m * 32 + r
    y = r // 8
    xc = lax.rem(r, 8)
    x = xc // 2
    core = lax.rem(xc, 2)
    sign = 1 - 2 * core
    mine = m * 8 + xc

    small = ((value_in, value), (precision_in, precision), (row_in, row), (patch_in, patch))

    def block(ch, t):
        return bg.at[ch, :, :, pl.ds(pl.multiple_of(t * 128, 128), 128)]

    def fetch(ch):
        @pl.loop(0, 32)
        def _(t):
            pltpu.make_async_copy(block(ch, t), stage.at[ch, t], in_sem.at[ch]).start()

        @pl.when(m == y)
        def _():
            pltpu.make_async_copy(block(ch, r), recv.at[ch, mine], recv_sem.at[ch]).start()

    barrier = pltpu.get_barrier_semaphore()

    @pl.loop(2, 6)
    def _(dz):
        tz = jnp.bitwise_and(m + dz, 3)
        for dy in (2, 3, 1, 0):
            ty = jnp.bitwise_and(y + dy, 3) * 8
            for dx in (2, 3, 1, 0):
                tx = ty + jnp.bitwise_and(x + dx, 3) * 2
                for dc in (1, 0):
                    def greet():
                        pl.semaphore_signal(
                            barrier, inc=1, device_id=(tz, tx + jnp.bitwise_xor(core, dc)), device_id_type=MESH)
                    if dy == dx == dc == 0:
                        pl.when(dz != 4)(greet)
                    else:
                        greet()

    @pl.loop(0, EARLY)
    def _(ch):
        fetch(ch)

    pltpu.make_async_copy(ens, lhs.at[pl.ds(0, K)], oself_sem).start()
    for n, (source, target) in enumerate(small):
        pltpu.make_async_copy(source, target, small_sem.at[n]).start()

    pl.semaphore_wait(barrier, ND - 1)

    def send(ch):
        pltpu.make_async_copy(recv.at[ch], stage.at[ch], in_sem.at[ch]).wait()

        @pl.loop(0, 32)
        def _(k):
            q = lax.rem(k * 7 + ch * 3, 32)
            tx = lax.rem(x + sign * lax.rem(q // 2, 4) + 8, 4)
            ty = lax.rem(y + sign * (q // 8) + 8 + m, 4)
            tc = lax.rem(core + lax.rem(q, 2), 2)
            t = (ty * 4 + tx) * 2 + tc

            @pl.when(jnp.logical_or(t != r, m != y))
            def _():
                pltpu.make_async_remote_copy(
                    src_ref=stage.at[ch, t], dst_ref=recv.at[ch, mine],
                    send_sem=send_sem.at[ch], recv_sem=recv_sem.at[ch],
                    device_id=(y, t), device_id_type=MESH).start()

    @pl.loop(0, EARLY)
    def _(ch):
        send(ch)

    @pl.loop(EARLY, C)
    def _(ch):
        fetch(ch)

    for n, (source, target) in enumerate(small):
        pltpu.make_async_copy(source, target, small_sem.at[n]).wait()

    above = lax.broadcasted_iota(jnp.int32, (512, 512), 0) < lax.broadcasted_iota(jnp.int32, (512, 512), 1)
    upper = jnp.where(above, 1.0, 0.0).astype(BF16)
    owner = lax.broadcasted_iota(jnp.int32, (ND, 128), 0)
    lane = lax.broadcasted_iota(jnp.int32, (128, 128), 1)

    def rank_block(b, before):
        rows = [patch[pl.ds(b * 4 + u, 1), :] for u in range(4)]
        hit = jnp.concatenate([jnp.where(owner == p, 1.0, 0.0) for p in rows], axis=1)
        count = jnp.dot(hit.astype(BF16), upper, preferred_element_type=F32) + before
        rank = jnp.sum(count * hit, axis=0, keepdims=True)
        for u in range(4):
            slot = rows[u].astype(F32) * CAP + rank[:, u * 128:(u + 1) * 128]
            column = jnp.broadcast_to(slot, (128, 128)).T.astype(jnp.int32)
            found = lane == jnp.bitwise_and(column, 127)
            key = jnp.where(found, jnp.right_shift(column, 7).astype(F32), -1.0)
            keys[pl.ds(pl.multiple_of((b * 4 + u) * 128, 128), 128), :] = key.astype(BF16)
        return before + jnp.sum(hit, axis=1, keepdims=True)

    lax.fori_loop(0, OBS // 512, rank_block, jnp.zeros((ND, 1), F32))

    lines[0] = value[...].astype(F32)
    lines[1] = precision[...].astype(F32)
    lines[2] = row[...].astype(F32)
    which = lax.broadcasted_iota(jnp.int32, (16, 128), 0)

    @pl.loop(0, OBS // 128)
    def _(i):
        at = pl.ds(pl.multiple_of(i * 128, 128), 128)
        one = pl.ds(i, 1)
        extra = jnp.where(which == 2, lines[2, one, :], 0.0)
        extra = jnp.where(which == 1, lines[1, one, :], extra)
        extra = jnp.where(which == 0, lines[0, one, :], extra)
        lhs[K:K + 16, at] = extra.astype(BF16)

    pltpu.make_async_copy(ens, lhs.at[pl.ds(0, K)], oself_sem).wait()

    half = lax.broadcasted_iota(jnp.int32, (32, 128), 1) < CAP
    half8 = lax.broadcasted_iota(jnp.int32, (8, 128), 1) < CAP

    line8 = lax.broadcasted_iota(jnp.int32, (8, 128), 0)

    def roll(v):
        return pltpu.roll(v, CAP, 1)

    @pl.loop(0, ND // 4)
    def _(g):
        total = jnp.zeros((K + 16, 256), F32)
        for kb in range(OBS // CHUNK):
            at = pl.ds(kb * CHUNK, CHUNK)
            key = keys[at, :]
            hot = [jnp.where(key == (2 * g + h).astype(F32).astype(BF16), 1.0, 0.0).astype(BF16) for h in range(2)]
            total += jnp.dot(lhs[:, at], jnp.concatenate(hot, axis=1), preferred_element_type=F32)
        for h in range(2):
            t = total[:, h * 128:(h + 1) * 128]
            low, high, more = t[0:32], t[32:64], t[64:72]
            swapped = roll(more)
            line = jnp.where(half8[0:1], more[0:1], swapped[1:2])
            tail = jnp.where(line8 == 0, line, jnp.where(half8, more[2:3], 0.0))
            first = jnp.concatenate([jnp.where(half, low, roll(high)), tail], axis=0)
            line = jnp.where(half8[0:1], swapped[0:1], more[1:2])
            tail = jnp.where(line8 == 0, line, jnp.where(half8, swapped[2:3], 0.0))
            second = jnp.concatenate([jnp.where(half, roll(low), high), tail], axis=0)
            obs_send[4 * g + 2 * h] = first.astype(BF16)
            obs_send[4 * g + 2 * h + 1] = second.astype(BF16)

    obs_recv[me] = obs_send[me]

    @pl.loop(1, ND)
    def _(d):
        to = lax.rem(me + lax.rem(d * 37, ND), ND)
        pltpu.make_async_remote_copy(
            src_ref=obs_send.at[to, pl.ds(0, SENT)], dst_ref=obs_recv.at[me, pl.ds(0, SENT)], send_sem=osend_sem, recv_sem=orecv_sem,
            device_id=(to // 32, lax.rem(to, 32)), device_id_type=MESH).start()

    @pl.loop(EARLY, MID)
    def _(ch):
        send(ch)

    gram[...] = jnp.zeros_like(gram)
    proj[...] = jnp.zeros_like(proj)
    others = obs_recv.at[pl.ds(0, ND - 1), pl.ds(0, SENT)]
    pltpu.make_async_copy(others, others, orecv_sem).wait()

    @pl.loop(MID, C)
    def _(ch):
        send(ch)

    centre = lax.broadcasted_iota(jnp.int32, (NB, 128), 0).astype(F32) * 2.0 + 0.5

    @pl.loop(0, ND // 2)
    def _(p):
        at = pl.ds(pl.multiple_of(p * 128, 128), 128)
        a = obs_recv[2 * p].astype(F32)
        b = obs_recv[2 * p + 1].astype(F32)
        low = jnp.where(half, a[0:32], roll(b[0:32]))
        high = jnp.where(half, roll(a[0:32]), b[0:32])
        here = half8[0:1]
        ea, eb = a[32:40], b[32:40]
        ra, rb = roll(ea), roll(eb)
        obs_val = jnp.where(here, ea[0:1], rb[0:1])
        obs_prec = jnp.where(here, ra[0:1], eb[0:1])
        obs_row = jnp.where(here, ea[1:2], rb[1:2])
        values = jnp.concatenate([low, high], axis=0)
        mean = jnp.sum(values, axis=0, keepdims=True) / K
        pert_t[:, at] = (values - mean).astype(BF16)
        distance = (obs_row - centre) / 12.0
        w = obs_prec * jnp.exp(-0.5 * distance * distance)
        weight[:, at] = w
        weighted[:, at] = w * (obs_val - mean)

    @pl.loop(0, ND * CAP // CHUNK)
    def _(kc):
        at = pl.ds(pl.multiple_of(kc * CHUNK, CHUNK), CHUNK)

        @pl.loop(0, NB)
        def _(j):
            w = weight[pl.ds(j, 1), at]
            scaled[pl.ds(pl.multiple_of(j * K, K), K), :] = (w * pert_t[:, at].astype(F32)).astype(BF16)

        gram[...] += nt(scaled[...], pert_t[:, at])
        proj[...] += nt(weighted[:, at], pert_t[:, at].astype(F32), precision=HI)

    eye = jnp.where(lax.broadcasted_iota(jnp.int32, (K, K), 0) == lax.broadcasted_iota(jnp.int32, (K, K), 1), 1.0, 0.0)

    def mm(a, b):
        return jnp.dot(a, b, precision=HI, preferred_element_type=F32)

    @pl.loop(0, NB // 4)
    def _(jj):
        group = range(4)
        sys_ = [gram[pl.ds(pl.multiple_of((jj * 4 + u) * K, K), K), :] + (K - 1.0) * eye for u in group]
        norm = [jnp.sqrt(jnp.sum(jnp.sum(s * s, axis=1, keepdims=True), axis=0, keepdims=True)) for s in sys_]
        root = [s / n for s, n in zip(sys_, norm)]
        middle = [1.5 * eye - 0.5 * a for a in root]
        root = [mm(a, b) for a, b in zip(root, middle)]
        inv = middle
        for step in range(1, NS_ITERS):
            middle = [1.5 * eye - 0.5 * mm(a, b) for a, b in zip(inv, root)]
            if step < NS_ITERS - 1:
                root = [mm(a, b) for a, b in zip(root, middle)]
            inv = [mm(a, b) for a, b in zip(middle, inv)]
        for u in group:
            inverse = mm(inv[u], inv[u]) / norm[u]
            shift = jnp.sum(inverse * proj[pl.ds(jj * 4 + u, 1), :], axis=1, keepdims=True)
            t = (jnp.sqrt((K - 1.0) / norm[u]) * inv[u] + shift)
            trans[jj * 4 + u] = t.T.astype(BF16)

    @pl.loop(0, C)
    def _(ch):
        pltpu.make_async_copy(stage.at[ch], recv.at[ch], recv_sem.at[ch]).wait()

        @pl.loop(0, 8, unroll=2)
        def _(s):
            for i in range(3):
                rows = [jnp.concatenate([recv[ch, z * 8 + s, 2 * i + h] for z in range(4)], axis=0) for h in range(2)]
                states = jnp.concatenate(rows, axis=1).astype(F32)
                mean = jnp.sum(states, axis=0, keepdims=True) / K
                anomaly = (states - mean).astype(BF16)
                result = jnp.dot(trans[s * 3 + i], anomaly, preferred_element_type=F32) + mean
                wide[pl.ds(s * 6 + 2 * i, K, stride=48), :] = result[:, 0:128]
                wide[pl.ds(s * 6 + 2 * i + 1, K, stride=48), :] = result[:, 128:256]

        @pl.loop(0, K // 8)
        def _(k):
            for u in range(8):
                out[k * 8 + u, ch] = wide[pl.ds((k * 8 + u) * 48, 48), :].astype(BF16)

    pltpu.make_async_copy(others, others, osend_sem).wait()

    @pl.loop(0, C)
    def _(ch):
        @pl.when(m == y)
        def _():
            part = recv.at[ch, pl.ds(0, 31)]
            pltpu.make_async_copy(part, part, send_sem.at[ch]).wait()

        @pl.when(m != y)
        def _():
            pltpu.make_async_copy(recv.at[ch], recv.at[ch], send_sem.at[ch]).wait()


def put(source, target, sem):
    @pl.loop(0, K // 4)
    def _(k):
        part = pl.ds(k * 4, 4)
        pltpu.make_async_copy(source.at[part], target.at[part], sem).start()

    pltpu.make_async_copy(source, target, sem).wait()


def local(background, obs_ens, obs_value, obs_precision, obs_row, obs_patch):
    lines = (OBS // 128, 128)
    operands = (
        background.transpose(1, 2, 0, 3), obs_ens.T, obs_value.reshape(lines), obs_precision.reshape(lines),
        obs_row.reshape(lines), obs_patch.reshape(lines),
    )
    vmem = pl.BlockSpec(memory_space=pltpu.VMEM)
    hbm = pl.BlockSpec(memory_space=pltpu.HBM)
    anyspace = pl.BlockSpec(memory_space=pl.ANY)
    result = pl.pallas_call(
        kernel,
        out_shape=jax.ShapeDtypeStruct((K, C, 48, 128), BF16),
        in_specs=[hbm] * 6,
        out_specs=vmem,
        scratch_shapes=[
            pltpu.VMEM((C, 32, ROWS, 16, 128), BF16),
            pltpu.VMEM((C, 32, ROWS, 16, 128), BF16),
            pltpu.VMEM(lines, BF16),
            pltpu.VMEM(lines, BF16),
            pltpu.VMEM(lines, jnp.int32),
            pltpu.VMEM(lines, jnp.int32),
            pltpu.VMEM((3, OBS // 128, 128), F32),
            pltpu.VMEM((K + 16, OBS), BF16),
            pltpu.VMEM((OBS, ND), BF16),
            pltpu.VMEM((ND, PIECE, 128), BF16),
            pltpu.VMEM((ND, PIECE, 128), BF16),
            pltpu.VMEM((K, ND * CAP), BF16),
            pltpu.VMEM((NB, ND * CAP), F32),
            pltpu.VMEM((NB, ND * CAP), F32),
            pltpu.VMEM((NB * K, CHUNK), BF16),
            pltpu.VMEM((NB * K, K), F32),
            pltpu.VMEM((NB, K), F32),
            pltpu.VMEM((NB, K, K), BF16),
            pltpu.VMEM((K * 48, 128), F32),
            pltpu.SemaphoreType.DMA((C,)),
            pltpu.SemaphoreType.DMA((C,)),
            pltpu.SemaphoreType.DMA((C,)),
            pltpu.SemaphoreType.DMA,
            pltpu.SemaphoreType.DMA,
            pltpu.SemaphoreType.DMA,
            pltpu.SemaphoreType.DMA((4,)),
        ],
        compiler_params=pltpu.CompilerParams(collective_id=0, has_side_effects=True, vmem_limit_bytes=42 * 2**20),
        name="analysis",
    )(*[pltpu.with_memory_space_constraint(o, pltpu.HBM) for o in operands])
    return pl.pallas_call(
        put,
        out_shape=jax.ShapeDtypeStruct((K, C, 48, 128), BF16),
        in_specs=[vmem],
        out_specs=anyspace,
        scratch_shapes=[pltpu.SemaphoreType.DMA],
        compiler_params=pltpu.CompilerParams(vmem_limit_bytes=2**20),
        name="put",
    )(result)


def solution(mesh):
    in_specs = (
        P("member", None, "region", None),
        P(("member", "region"), None),
        P(("member", "region")),
        P(("member", "region")),
        P(("member", "region")),
        P(("member", "region"), None),
    )
    out_specs = P(None, None, "member", "region")
    return jax.shard_map(local, mesh=mesh, in_specs=in_specs, out_specs=out_specs, check_vma=False)
```

```python
import jax
import jax.numpy as jnp
from jax import lax
from jax.experimental import pallas as pl
from jax.experimental.pallas import tpu as pltpu
from jax.sharding import PartitionSpec as P

MESH = pl.DeviceIdType.MESH
F32 = jnp.float32
BF16 = jnp.bfloat16
HI = lax.Precision.HIGHEST

K = 64
C = 13
ROWS = 6
LON = 4096
OBS = 4096
CAP = 64
NB = 24
ND = 128
NS_ITERS = 4
EARLY = 4
MID = 5
PIECE = 40
SENT = 34
CHUNK = 1024


def nt(a, b, **kw):
    return lax.dot_general(a, b, (((1,), (1,)), ((), ())), preferred_element_type=F32, **kw)


def kernel(bg, ens, value_in, precision_in, row_in, patch_in, out, stage, recv, value, precision, row, patch, lines, lhs, keys, obs_send, obs_recv, pert_t, weight, weighted,
           scaled, gram, proj, trans, wide, in_sem, send_sem, recv_sem, osend_sem, orecv_sem, oself_sem, small_sem):
    m = lax.axis_index("member")
    r = lax.axis_index("region")
    me = m * 32 + r
    y = r // 8
    xc = lax.rem(r, 8)
    x = xc // 2
    core = lax.rem(xc, 2)
    sign = 1 - 2 * core
    mine = m * 8 + xc

    small = ((value_in, value), (precision_in, precision), (row_in, row), (patch_in, patch))

    def block(ch, t):
        return bg.at[ch, :, :, pl.ds(pl.multiple_of(t * 128, 128), 128)]

    def fetch(ch):
        @pl.loop(0, 32)
        def _(t):
            pltpu.make_async_copy(block(ch, t), stage.at[ch, t], in_sem.at[ch]).start()

        @pl.when(m == y)
        def _():
            pltpu.make_async_copy(block(ch, r), recv.at[ch, mine], recv_sem.at[ch]).start()

    barrier = pltpu.get_barrier_semaphore()

    @pl.loop(2, 6)
    def _(dz):
        tz = jnp.bitwise_and(m + dz, 3)
        for dy in (2, 3, 1, 0):
            ty = jnp.bitwise_and(y + dy, 3) * 8
            for dx in (2, 3, 1, 0):
                tx = ty + jnp.bitwise_and(x + dx, 3) * 2
                for dc in (1, 0):
                    def greet():
                        pl.semaphore_signal(
                            barrier, inc=1, device_id=(tz, tx + jnp.bitwise_xor(core, dc)), device_id_type=MESH)
                    if dy == dx == dc == 0:
                        pl.when(dz != 4)(greet)
                    else:
                        greet()

    @pl.loop(0, EARLY)
    def _(ch):
        fetch(ch)

    pltpu.make_async_copy(ens, lhs.at[pl.ds(0, K)], oself_sem).start()
    for n, (source, target) in enumerate(small):
        pltpu.make_async_copy(source, target, small_sem.at[n]).start()

    pl.semaphore_wait(barrier, ND - 1)

    def send(ch):
        pltpu.make_async_copy(recv.at[ch], stage.at[ch], in_sem.at[ch]).wait()

        @pl.loop(0, 32)
        def _(k):
            q = lax.rem(k * 7 + ch * 3, 32)
            tx = lax.rem(x + sign * lax.rem(q // 2, 4) + 8, 4)
            ty = lax.rem(y + sign * (q // 8) + 8 + m, 4)
            tc = lax.rem(core + lax.rem(q, 2), 2)
            t = (ty * 4 + tx) * 2 + tc

            @pl.when(jnp.logical_or(t != r, m != y))
            def _():
                pltpu.make_async_remote_copy(
                    src_ref=stage.at[ch, t], dst_ref=recv.at[ch, mine],
                    send_sem=send_sem.at[ch], recv_sem=recv_sem.at[ch],
                    device_id=(y, t), device_id_type=MESH).start()

    @pl.loop(0, EARLY)
    def _(ch):
        send(ch)

    @pl.loop(EARLY, C)
    def _(ch):
        fetch(ch)

    for n, (source, target) in enumerate(small):
        pltpu.make_async_copy(source, target, small_sem.at[n]).wait()

    above = lax.broadcasted_iota(jnp.int32, (512, 512), 0) < lax.broadcasted_iota(jnp.int32, (512, 512), 1)
    upper = jnp.where(above, 1.0, 0.0).astype(BF16)
    owner = lax.broadcasted_iota(jnp.int32, (ND, 128), 0)
    lane = lax.broadcasted_iota(jnp.int32, (128, 128), 1)

    def rank_block(b, before):
        rows = [patch[pl.ds(b * 4 + u, 1), :] for u in range(4)]
        hit = jnp.concatenate([jnp.where(owner == p, 1.0, 0.0) for p in rows], axis=1)
        count = jnp.dot(hit.astype(BF16), upper, preferred_element_type=F32) + before
        rank = jnp.sum(count * hit, axis=0, keepdims=True)
        for u in range(4):
            slot = rows[u].astype(F32) * CAP + rank[:, u * 128:(u + 1) * 128]
            column = jnp.broadcast_to(slot, (128, 128)).T.astype(jnp.int32)
            found = lane == jnp.bitwise_and(column, 127)
            key = jnp.where(found, jnp.right_shift(column, 7).astype(F32), -1.0)
            keys[pl.ds(pl.multiple_of((b * 4 + u) * 128, 128), 128), :] = key.astype(BF16)
        return before + jnp.sum(hit, axis=1, keepdims=True)

    lax.fori_loop(0, OBS // 512, rank_block, jnp.zeros((ND, 1), F32))

    lines[0] = value[...].astype(F32)
    lines[1] = precision[...].astype(F32)
    lines[2] = row[...].astype(F32)
    which = lax.broadcasted_iota(jnp.int32, (16, 128), 0)

    @pl.loop(0, OBS // 128)
    def _(i):
        at = pl.ds(pl.multiple_of(i * 128, 128), 128)
        one = pl.ds(i, 1)
        extra = jnp.where(which == 2, lines[2, one, :], 0.0)
        extra = jnp.where(which == 1, lines[1, one, :], extra)
        extra = jnp.where(which == 0, lines[0, one, :], extra)
        lhs[K:K + 16, at] = extra.astype(BF16)

    pltpu.make_async_copy(ens, lhs.at[pl.ds(0, K)], oself_sem).wait()

    half = lax.broadcasted_iota(jnp.int32, (32, 128), 1) < CAP
    half8 = lax.broadcasted_iota(jnp.int32, (8, 128), 1) < CAP

    line8 = lax.broadcasted_iota(jnp.int32, (8, 128), 0)

    def roll(v):
        return pltpu.roll(v, CAP, 1)

    @pl.loop(0, ND // 4)
    def _(g):
        total = jnp.zeros((K + 16, 256), F32)
        for kb in range(OBS // CHUNK):
            at = pl.ds(kb * CHUNK, CHUNK)
            key = keys[at, :]
            hot = [jnp.where(key == (2 * g + h).astype(F32).astype(BF16), 1.0, 0.0).astype(BF16) for h in range(2)]
            total += jnp.dot(lhs[:, at], jnp.concatenate(hot, axis=1), preferred_element_type=F32)
        for h in range(2):
            t = total[:, h * 128:(h + 1) * 128]
            low, high, more = t[0:32], t[32:64], t[64:72]
            swapped = roll(more)
            line = jnp.where(half8[0:1], more[0:1], swapped[1:2])
            tail = jnp.where(line8 == 0, line, jnp.where(half8, more[2:3], 0.0))
            first = jnp.concatenate([jnp.where(half, low, roll(high)), tail], axis=0)
            line = jnp.where(half8[0:1], swapped[0:1], more[1:2])
            tail = jnp.where(line8 == 0, line, jnp.where(half8, swapped[2:3], 0.0))
            second = jnp.concatenate([jnp.where(half, roll(low), high), tail], axis=0)
            obs_send[4 * g + 2 * h] = first.astype(BF16)
            obs_send[4 * g + 2 * h + 1] = second.astype(BF16)

    obs_recv[me] = obs_send[me]

    @pl.loop(1, ND)
    def _(d):
        to = lax.rem(me + lax.rem(d * 37, ND), ND)
        pltpu.make_async_remote_copy(
            src_ref=obs_send.at[to, pl.ds(0, SENT)], dst_ref=obs_recv.at[me, pl.ds(0, SENT)], send_sem=osend_sem, recv_sem=orecv_sem,
            device_id=(to // 32, lax.rem(to, 32)), device_id_type=MESH).start()

    @pl.loop(EARLY, MID)
    def _(ch):
        send(ch)

    gram[...] = jnp.zeros_like(gram)
    proj[...] = jnp.zeros_like(proj)
    others = obs_recv.at[pl.ds(0, ND - 1), pl.ds(0, SENT)]
    pltpu.make_async_copy(others, others, orecv_sem).wait()

    @pl.loop(MID, C)
    def _(ch):
        send(ch)

    centre = lax.broadcasted_iota(jnp.int32, (NB, 128), 0).astype(F32) * 2.0 + 0.5

    @pl.loop(0, ND // 2)
    def _(p):
        at = pl.ds(pl.multiple_of(p * 128, 128), 128)
        a = obs_recv[2 * p].astype(F32)
        b = obs_recv[2 * p + 1].astype(F32)
        low = jnp.where(half, a[0:32], roll(b[0:32]))
        high = jnp.where(half, roll(a[0:32]), b[0:32])
        here = half8[0:1]
        ea, eb = a[32:40], b[32:40]
        ra, rb = roll(ea), roll(eb)
        obs_val = jnp.where(here, ea[0:1], rb[0:1])
        obs_prec = jnp.where(here, ra[0:1], eb[0:1])
        obs_row = jnp.where(here, ea[1:2], rb[1:2])
        values = jnp.concatenate([low, high], axis=0)
        mean = jnp.sum(values, axis=0, keepdims=True) / K
        pert_t[:, at] = (values - mean).astype(BF16)
        distance = (obs_row - centre) / 12.0
        w = obs_prec * jnp.exp(-0.5 * distance * distance)
        weight[:, at] = w
        weighted[:, at] = w * (obs_val - mean)

    @pl.loop(0, ND * CAP // CHUNK)
    def _(kc):
        at = pl.ds(pl.multiple_of(kc * CHUNK, CHUNK), CHUNK)

        @pl.loop(0, NB)
        def _(j):
            w = weight[pl.ds(j, 1), at]
            scaled[pl.ds(pl.multiple_of(j * K, K), K), :] = (w * pert_t[:, at].astype(F32)).astype(BF16)

        gram[...] += nt(scaled[...], pert_t[:, at])
        proj[...] += nt(weighted[:, at], pert_t[:, at].astype(F32), precision=HI)

    eye = jnp.where(lax.broadcasted_iota(jnp.int32, (K, K), 0) == lax.broadcasted_iota(jnp.int32, (K, K), 1), 1.0, 0.0)

    def mm(a, b):
        return jnp.dot(a, b, precision=HI, preferred_element_type=F32)

    @pl.loop(0, NB // 4)
    def _(jj):
        group = range(4)
        sys_ = [gram[pl.ds(pl.multiple_of((jj * 4 + u) * K, K), K), :] + (K - 1.0) * eye for u in group]
        norm = [jnp.sqrt(jnp.sum(jnp.sum(s * s, axis=1, keepdims=True), axis=0, keepdims=True)) for s in sys_]
        root = [s / n for s, n in zip(sys_, norm)]
        middle = [1.5 * eye - 0.5 * a for a in root]
        root = [mm(a, b) for a, b in zip(root, middle)]
        inv = middle
        for step in range(1, NS_ITERS):
            middle = [1.5 * eye - 0.5 * mm(a, b) for a, b in zip(inv, root)]
            if step < NS_ITERS - 1:
                root = [mm(a, b) for a, b in zip(root, middle)]
            inv = [mm(a, b) for a, b in zip(middle, inv)]
        for u in group:
            inverse = mm(inv[u], inv[u]) / norm[u]
            shift = jnp.sum(inverse * proj[pl.ds(jj * 4 + u, 1), :], axis=1, keepdims=True)
            t = (jnp.sqrt((K - 1.0) / norm[u]) * inv[u] + shift)
            trans[jj * 4 + u] = t.T.astype(BF16)

    @pl.loop(0, C)
    def _(ch):
        pltpu.make_async_copy(stage.at[ch], recv.at[ch], recv_sem.at[ch]).wait()

        @pl.loop(0, 8, unroll=2)
        def _(s):
            for i in range(3):
                rows = [jnp.concatenate([recv[ch, z * 8 + s, 2 * i + h] for z in range(4)], axis=0) for h in range(2)]
                states = jnp.concatenate(rows, axis=1).astype(F32)
                mean = jnp.sum(states, axis=0, keepdims=True) / K
                anomaly = (states - mean).astype(BF16)
                result = jnp.dot(trans[s * 3 + i], anomaly, preferred_element_type=F32) + mean
                wide[pl.ds(s * 6 + 2 * i, K, stride=48), :] = result[:, 0:128]
                wide[pl.ds(s * 6 + 2 * i + 1, K, stride=48), :] = result[:, 128:256]

        @pl.loop(0, K // 8)
        def _(k):
            for u in range(8):
                out[k * 8 + u, ch] = wide[pl.ds((k * 8 + u) * 48, 48), :].astype(BF16)

    pltpu.make_async_copy(others, others, osend_sem).wait()

    @pl.loop(0, C)
    def _(ch):
        @pl.when(m == y)
        def _():
            part = recv.at[ch, pl.ds(0, 31)]
            pltpu.make_async_copy(part, part, send_sem.at[ch]).wait()

        @pl.when(m != y)
        def _():
            pltpu.make_async_copy(recv.at[ch], recv.at[ch], send_sem.at[ch]).wait()


def put(source, target, sem):
    @pl.loop(0, K // 4)
    def _(k):
        part = pl.ds(k * 4, 4)
        pltpu.make_async_copy(source.at[part], target.at[part], sem).start()

    pltpu.make_async_copy(source, target, sem).wait()


def local(background, obs_ens, obs_value, obs_precision, obs_row, obs_patch):
    lines = (OBS // 128, 128)
    operands = (
        background.transpose(1, 2, 0, 3), obs_ens.T, obs_value.reshape(lines), obs_precision.reshape(lines),
        obs_row.reshape(lines), obs_patch.reshape(lines),
    )
    vmem = pl.BlockSpec(memory_space=pltpu.VMEM)
    hbm = pl.BlockSpec(memory_space=pltpu.HBM)
    anyspace = pl.BlockSpec(memory_space=pl.ANY)
    result = pl.pallas_call(
        kernel,
        out_shape=jax.ShapeDtypeStruct((K, C, 48, 128), BF16),
        in_specs=[hbm] * 6,
        out_specs=vmem,
        scratch_shapes=[
            pltpu.VMEM((C, 32, ROWS, 16, 128), BF16),
            pltpu.VMEM((C, 32, ROWS, 16, 128), BF16),
            pltpu.VMEM(lines, BF16),
            pltpu.VMEM(lines, BF16),
            pltpu.VMEM(lines, jnp.int32),
            pltpu.VMEM(lines, jnp.int32),
            pltpu.VMEM((3, OBS // 128, 128), F32),
            pltpu.VMEM((K + 16, OBS), BF16),
            pltpu.VMEM((OBS, ND), BF16),
            pltpu.VMEM((ND, PIECE, 128), BF16),
            pltpu.VMEM((ND, PIECE, 128), BF16),
            pltpu.VMEM((K, ND * CAP), BF16),
            pltpu.VMEM((NB, ND * CAP), F32),
            pltpu.VMEM((NB, ND * CAP), F32),
            pltpu.VMEM((NB * K, CHUNK), BF16),
            pltpu.VMEM((NB * K, K), F32),
            pltpu.VMEM((NB, K), F32),
            pltpu.VMEM((NB, K, K), BF16),
            pltpu.VMEM((K * 48 + 48, 128), F32),
            pltpu.SemaphoreType.DMA((C,)),
            pltpu.SemaphoreType.DMA((C,)),
            pltpu.SemaphoreType.DMA((C,)),
            pltpu.SemaphoreType.DMA,
            pltpu.SemaphoreType.DMA,
            pltpu.SemaphoreType.DMA,
            pltpu.SemaphoreType.DMA((4,)),
        ],
        compiler_params=pltpu.CompilerParams(collective_id=0, has_side_effects=True, vmem_limit_bytes=42 * 2**20),
        name="analysis",
    )(*[pltpu.with_memory_space_constraint(o, pltpu.HBM) for o in operands])
    return pl.pallas_call(
        put,
        out_shape=jax.ShapeDtypeStruct((K, C, 48, 128), BF16),
        in_specs=[vmem],
        out_specs=anyspace,
        scratch_shapes=[pltpu.SemaphoreType.DMA],
        compiler_params=pltpu.CompilerParams(vmem_limit_bytes=2**20),
        name="put",
    )(result)


def solution(mesh):
    in_specs = (
        P("member", None, "region", None),
        P(("member", "region"), None),
        P(("member", "region")),
        P(("member", "region")),
        P(("member", "region")),
        P(("member", "region"), None),
    )
    out_specs = P(None, None, "member", "region")
    return jax.shard_map(local, mesh=mesh, in_specs=in_specs, out_specs=out_specs, check_vma=False)
```
